256 devices in a mesh: rows: 64 (over x, z_hi, y, core), feat: 4 (over z_lo).
Axes of the slice: x: 4, y: 4, z: 8 (z_hi: 2, z_lo: 4; z = z_hi * 4 + z_lo), core: 2. Of those that a mesh axis runs over, the one named last changes fastest.
Arguments:
- bins: int32 [65536, 512], P('rows', 'feat'), may hold values from -2147483648 to 2147483647, as said below
- hessian: float32 [262144], P('rows'), may hold values from 0.05 to 1
- thresholds: float32 [128], replicated, may hold values from 0.02 to 0.98
Outputs:
- cuts: float32 [512, 128], P('feat')
The draws below stay inside these ranges and needn't reach their ends.
Inputs may be any that keep to these rules, and one draw needn't show every extreme that they name: `bins`: each word holds the bin ids, 0 to 255, of rows 4i to 4i + 3 of one feature, row 4i + k in bits 8k to 8k + 7 of the two's complement word.
All inputs are finite; a program needn't handle non-finite values.
Results may differ from the reference program's by a relative error of at most 0.000065.
Values sent between devices are 32-bit elements; how exact they have to be, the bound alone decides.
A program may use at most 192 MiB of HBM per device.

```python
import math
import jax
import jax.numpy as jnp

F = 512
BINS = 256
Q = 128
ROW_DEV = 4096
ROWS = 262144
N_ROWS = 64


def draw_bins(key, part):
    key = jax.random.fold_in(key, 17)
    first, second, third, fourth = jax.random.split(key, 4)
    spread = jax.random.randint(first, (ROWS, F), 0, BINS)
    centers = jax.random.randint(second, (N_ROWS, F), 0, BINS)
    offsets = jax.random.randint(third, (ROWS, F), 0, 8)
    banded = jax.random.randint(fourth, (ROWS, F), 0, 2) == 0
    owner = jnp.arange(ROWS, dtype=jnp.int32) // ROW_DEV
    center_rows = centers[owner]
    ids = jnp.where(banded, (center_rows + offsets) % BINS, spread).astype(jnp.int32)
    grouped = ids.reshape(ROWS // 4, 4, F)
    packed = jnp.zeros((ROWS // 4, F), jnp.int32)
    for k in range(4):
        packed = jnp.bitwise_or(packed, jnp.left_shift(grouped[:, k, :], 8 * k))
    return packed.astype(jnp.int32)


def block_levels(own_key, dims, pieces, least, largest):
    loudness = 1.0
    for dim, shards_of in pieces:
        heights = jax.random.uniform(jax.random.fold_in(jax.random.fold_in(own_key, 6), dim), (shards_of,), jnp.float32, least / len(pieces), largest / len(pieces))
        loudness = loudness * jnp.repeat(jnp.exp(heights), dims[dim] // shards_of).reshape((-1,) + (1,) * (len(dims) - 1 - dim))
    return loudness


def setup_inputs(seed: int = 0) -> dict:
    key_list = jax.random.split(jax.random.key(seed), 4)
    return {
        "bins": draw_bins(jax.random.fold_in(key_list[3], 71), 0),
        "hessian": jnp.clip(jnp.exp(math.log(1.0) - 2.9957323 * jax.random.uniform(key_list[1], (ROWS,), jnp.float32) ** block_levels(key_list[1], (ROWS,), ((0, 64),), -0.2, 0.2)), 0.05, 1.0),
        "thresholds": jnp.clip(jax.random.uniform(key_list[2], (Q,), jnp.float32, 0.02, 0.98), 0.02, 0.98),
    }


def unpack(words):
    parts = [jnp.bitwise_and(jnp.right_shift(words, 8 * k), 255) for k in range(4)]
    stacked = jnp.stack(parts, axis=1)
    return stacked.reshape(words.shape[0] * 4, words.shape[1]).astype(jnp.int32)


def cut_positions(hist, thresholds):
    cum = jnp.cumsum(hist, axis=1)
    before = cum - hist
    total = cum[:, -1]
    target = thresholds[None, :, None] * total[:, None, None]
    ratio = (target - before[:, None, :]) / (hist[:, None, :] + 1.0)
    return jnp.sum(jnp.clip(ratio, 0.0, 1.0), axis=2)


def reference(bins, hessian, thresholds):
    ids = unpack(bins)

    def one_feature(column):
        return jax.ops.segment_sum(hessian, column, num_segments=BINS)

    hist = jax.vmap(one_feature)(ids.T).astype(jnp.float32)
    return cut_positions(hist, thresholds)
```

```python
import jax
import jax.numpy as jnp
from jax import lax
from jax.experimental import pallas as pl
from jax.experimental.pallas import tpu as pltpu
from jax.sharding import PartitionSpec as P

LEVELS = 16
GROUP = 16
OCTET = 8
LANES = 128
CHUNK = 256
NX, NZ, NY, NC = 4, 2, 4, 2
RANKS = NX * NZ * NY * NC
SEATS = NX * NY
STEPS = SEATS // 2
MESH = pl.DeviceIdType.MESH


def kernel(bins_hbm, hess_hbm, thr_hbm, out_ref, bins_ref, hess_ref, thr_ref, prefix, column_ref, cols, wts, stage, inbox, mine, load_sem, send_sem, recv_sem, gather_send, gather_recv):
    words, width = bins_ref.shape
    tiles = words // LANES
    hess_load = pltpu.make_async_copy(hess_hbm, hess_ref, load_sem.at[tiles])
    hess_load.start()
    bins_loads = []
    for t in range(tiles):
        part = pl.ds(t * LANES, LANES)
        bins_loads.append(pltpu.make_async_copy(bins_hbm.at[part, :], bins_ref.at[part, :], load_sem.at[t]))
        bins_loads[t].start()
    thr_load = pltpu.make_async_copy(thr_hbm, thr_ref, load_sem.at[tiles + 1])
    thr_load.start()
    me = lax.axis_index("rows")
    x, z, y, core = me // (NZ * NY * NC), me // (NY * NC) % NZ, me // NC % NY, me % NC
    owner = core == NC - 1

    def device(px, pz, py, pc):
        return ((px * NZ + pz) * NY + py) * NC + pc

    barrier = pltpu.get_barrier_semaphore()
    for step in range(1, RANKS):
        pl.semaphore_signal(barrier, inc=1, device_id={"rows": (me + step) % RANKS}, device_id_type=MESH)

    src = lax.broadcasted_iota(jnp.int32, (LANES, LANES), 0)
    dst = lax.broadcasted_iota(jnp.int32, (LANES, LANES), 1)
    gap = dst - src
    same = jnp.bitwise_and(gap, OCTET - 1) == 0
    prefix[:, :LANES] = jnp.where(jnp.logical_and(same, gap > 0), 1.0, 0.0).astype(jnp.bfloat16)
    prefix[:, LANES:] = jnp.where(same, 1.0, 0.0).astype(jnp.bfloat16)

    quarter = LANES // 4
    order = jnp.where(src == 4 * (dst % quarter) + dst // quarter, 1.0, 0.0).astype(jnp.bfloat16)
    lane = lax.broadcasted_iota(jnp.int32, (2 * tiles, LANES), 1) // quarter
    hess_load.wait()
    flat = jnp.concatenate([hess_ref[pl.ds(j, tiles, stride=4), :] for j in range(4)], axis=0)
    left_factor = jnp.ones_like(flat)
    miss = jnp.abs(flat - flat.astype(jnp.bfloat16).astype(jnp.float32))
    for j in range(1, 128, 2):
        factor = 1.0 + j / 128.0
        other = (flat * (1.0 / factor)).astype(jnp.bfloat16).astype(jnp.float32)
        away = jnp.abs(flat - other * factor)
        left_factor = jnp.where(away < miss, factor, left_factor)
        miss = jnp.minimum(miss, away)
    right_factor = flat / left_factor
    for t in range(tiles):
        bins_loads[t].wait()
    thr_load.wait()
    for t in range(tiles):
        cols[:, t * LANES : (t + 1) * LANES] = bins_ref[t * LANES : (t + 1) * LANES, :].T
    column_ref[...] = jnp.broadcast_to(thr_ref[...], (LANES, thr_ref.shape[1])).T
    pieces = jnp.concatenate([x[j * tiles : (j + 1) * tiles] for j in range(4) for x in (left_factor, right_factor)], axis=0)
    moved = jnp.dot(pieces.astype(jnp.bfloat16), order, preferred_element_type=jnp.float32)
    for k in range(4):
        plane = None
        for j in range(4):
            block = moved[2 * tiles * j : 2 * tiles * (j + 1)]
            if j != k:
                block = pltpu.roll(block, (quarter * (j - k)) % LANES, 1)
            plane = block if plane is None else jnp.where(lane == j, block, plane)
        for piece in range(2):
            for t in range(tiles):
                line = plane[piece * tiles + t : piece * tiles + t + 1]
                wts[piece, k, :, t * LANES : (t + 1) * LANES] = jnp.broadcast_to(line, (GROUP, LANES)).astype(jnp.bfloat16)

    sub = lax.broadcasted_iota(jnp.int32, (OCTET, LANES), 0)
    diagonal = sub == lax.broadcasted_iota(jnp.int32, (OCTET, LANES), 1) % OCTET

    def gather_rows(tiles8):
        low4, low2, low1 = sub < 4, sub % 4 < 2, sub % 2 < 1
        four = []
        for a in range(4):
            p, q = tiles8[a], tiles8[a + 4]
            four.append(jnp.where(low4, p, q) + pltpu.roll(jnp.where(low4, q, p), 4, 0))
        two = []
        for a in range(2):
            p, q = four[a], four[a + 2]
            two.append(jnp.where(low2, p, q) + jnp.where(low2, pltpu.roll(p, 6, 0), pltpu.roll(q, 2, 0)))
        p, q = two
        return jnp.where(low1, p, q) + jnp.where(low1, pltpu.roll(p, 7, 0), pltpu.roll(q, 1, 0))

    def group_hist(group):
        base = pl.multiple_of(group * GROUP, GROUP)
        zero = jnp.zeros((GROUP, CHUNK), jnp.bfloat16)
        upper = (lax.broadcasted_iota(jnp.int32, (GROUP, CHUNK), 0) // OCTET)
        sums = [None, None]
        index = 0
        for c in range(words // CHUNK):
            part = cols[pl.ds(base, GROUP), c * CHUNK : (c + 1) * CHUNK]
            for k in range(4):
                high = jnp.bitwise_and(jnp.right_shift(part, 8 * k + 4), 15).astype(jnp.float32).astype(jnp.bfloat16)
                low = jnp.bitwise_and(jnp.right_shift(part, 8 * k), 15)
                w0 = wts[0, k, :, c * CHUNK : (c + 1) * CHUNK]
                w1 = wts[1, k, :, c * CHUNK : (c + 1) * CHUNK]
                left = jnp.concatenate([jnp.where(high == jnp.bfloat16(h), w0, zero) for h in range(LEVELS)], axis=0)
                rights = []
                for o in range(2):
                    eight = low[o * OCTET : (o + 1) * OCTET]
                    pair = (jnp.concatenate([eight, eight], axis=0) - upper).astype(jnp.float32).astype(jnp.bfloat16)
                    rights += [jnp.where(pair == jnp.bfloat16(l), w1, zero) for l in range(0, LEVELS, 2)]
                right = jnp.concatenate(rights, axis=0)
                part_sum = lax.dot_general(left, right, (((1,), (1,)), ((), ())), preferred_element_type=jnp.float32)
                side = index % 2
                sums[side] = part_sum if sums[side] is None else sums[side] + part_sum
                index += 1
        joint = sums[0] + sums[1]
        blocks = []
        for o in range(2):
            cut = slice(o * LANES, (o + 1) * LANES)
            rows = [joint[h * GROUP + o * OCTET : h * GROUP + (o + 1) * OCTET, cut] for h in range(LEVELS)]
            rows = [jnp.where(diagonal, r, 0.0) for r in rows]
            blocks.append(jnp.concatenate([gather_rows(rows[:8]), gather_rows(rows[8:])], axis=0))
        return blocks

    def shift_x(turn):
        return (2 + 3 * turn + 3 * (turn * (turn - 1) // 2)) % NX

    def target_of(step_x, step_y, o, far):
        return device((x + step_x) % NX, (z + far) % NZ, (y // 2 + step_y) % 2 * 2 + o, NC - 1)

    def outgoing(turn, half, o, far):
        target = target_of(shift_x(turn), 1 - half, o, far)
        return pltpu.make_async_remote_copy(
            src_ref=stage.at[2 * turn + half, o],
            dst_ref=inbox.at[(me - target + RANKS) % RANKS],
            send_sem=send_sem.at[0],
            recv_sem=recv_sem.at[0],
            device_id={"rows": target},
            device_id_type=MESH,
        )

    turns = STEPS // 2

    def do_pair(turn, carry):
        for half in range(2):
            group = (x + shift_x(turn)) % NX * 2 + (y // 2 + 1 - half) % 2
            for o, block in enumerate(group_hist(group)):
                stage[2 * turn + half, o] = block

        @pl.when(turn == 0)
        def _():
            pl.semaphore_wait(barrier, RANKS - 1)

        for far in (1, 0):
            for half in range(2):
                for o in range(2):
                    itself = owner & (turn == turns - 1) & (y % 2 == o) if half == 1 and far == 0 else None
                    if itself is None:
                        outgoing(turn, half, o, far).start()
                    else:
                        @pl.when(jnp.logical_not(itself))
                        def _():
                            outgoing(turn, half, o, far).start()

        return carry

    lax.fori_loop(0, turns, do_pair, 0)

    def spread(k):
        target = device((x + k // (NY * NC)) % NX, z, (y + k // NC % NY) % NY, (core + k % NC) % NC)
        return pltpu.make_async_remote_copy(
            src_ref=mine,
            dst_ref=out_ref.at[pl.ds(here, OCTET), :],
            send_sem=gather_send.at[0],
            recv_sem=gather_recv.at[0],
            device_id={"rows": target},
            device_id_type=MESH,
        )

    def drain(ref, sem):
        return pltpu.make_async_copy(ref, ref, sem.at[0])

    here = pl.multiple_of((x * NY + y) * OCTET, OCTET)

    @pl.when(owner)
    def _():
        drain(inbox.at[pl.ds(0, RANKS - 1)], recv_sem).wait()
        sums = [stage[STEPS - 1, y % 2], None, None, None]
        for s in range(1, RANKS):
            part = inbox[s]
            sums[s % 4] = part if sums[s % 4] is None else sums[s % 4] + part
        total = (sums[0] + sums[1]) + (sums[2] + sums[3])

        p0 = total.astype(jnp.bfloat16).astype(jnp.float32)
        p1 = (total - p0).astype(jnp.bfloat16).astype(jnp.float32)
        p2 = total - p0 - p1
        split = jnp.concatenate([p0, p1, p2], axis=0).astype(jnp.bfloat16)
        sums3 = jnp.dot(split, prefix[...], preferred_element_type=jnp.float32)
        joined = sums3[:LEVELS] + sums3[LEVELS : 2 * LEVELS] + sums3[2 * LEVELS :]
        inner, level = joined[:, :LANES], joined[:, LANES:]
        inv = 1.0 / (total + 1.0)
        whole = jnp.sum(level, axis=0, keepdims=True)
        target = column_ref[...] * whole
        run = jnp.zeros((1, LANES), jnp.float32)
        acc = jnp.zeros((thr_ref.shape[1], LANES), jnp.float32)
        for h in range(LEVELS):
            before = inner[h : h + 1] + run
            run = run + level[h : h + 1]
            ratio = (target - before) * inv[h : h + 1]
            acc = acc + jnp.clip(ratio, 0.0, 1.0)
        turned = acc.T
        cuts = turned[:OCTET]
        for j in range(1, LANES // OCTET):
            cuts = cuts + turned[j * OCTET : (j + 1) * OCTET]
        mine[...] = cuts
        for k in reversed(range(1, SEATS * NC)):
            spread(k).start()
        out_ref[pl.ds(here, OCTET), :] = cuts
        drain(inbox.at[pl.ds(0, 2 * SEATS - 1)], send_sem).wait()
        drain(out_ref.at[pl.ds(0, (SEATS - 1) * OCTET), :], gather_recv).wait()
        for k in range(1, SEATS * NC):
            spread(k).wait_send()

    @pl.when(jnp.logical_not(owner))
    def _():
        drain(inbox.at[pl.ds(0, 2 * SEATS)], send_sem).wait()
        drain(out_ref, gather_recv).wait()


def solution(mesh):
    def local(bins, hessian, thresholds):
        words, width = bins.shape
        quantiles = thresholds.shape[0]
        return pl.pallas_call(
            kernel,
            out_shape=pltpu.VMEM((width, quantiles), jnp.float32),
            in_specs=[pl.BlockSpec(memory_space=pl.ANY)] * 3,
            out_specs=pl.BlockSpec(memory_space=pltpu.VMEM),
            scratch_shapes=[
                pltpu.VMEM((words, width), jnp.int32),
                pltpu.VMEM((4 * words // LANES, LANES), jnp.float32),
                pltpu.VMEM((1, quantiles), jnp.float32),
                pltpu.VMEM((LANES, 2 * LANES), jnp.bfloat16),
                pltpu.VMEM((quantiles, LANES), jnp.float32),
                pltpu.VMEM((width, words), jnp.int32),
                pltpu.VMEM((2, 4, GROUP, words), jnp.bfloat16),
                pltpu.VMEM((STEPS, 2, LEVELS, LANES), jnp.float32),
                pltpu.VMEM((RANKS, LEVELS, LANES), jnp.float32),
                pltpu.VMEM((OCTET, quantiles), jnp.float32),
                pltpu.SemaphoreType.DMA((words // LANES + 2,)),
                pltpu.SemaphoreType.DMA((1,)),
                pltpu.SemaphoreType.DMA((1,)),
                pltpu.SemaphoreType.DMA((1,)),
                pltpu.SemaphoreType.DMA((1,)),
            ],
            compiler_params=pltpu.CompilerParams(collective_id=0, has_side_effects=True),
        )(bins, hessian.reshape(-1, LANES), thresholds.reshape(1, -1))

    in_specs = (P("rows", "feat"), P("rows"), P())
    return jax.shard_map(local, mesh=mesh, in_specs=in_specs, out_specs=P("feat", None), check_vma=False)
```

```python
import jax
import jax.numpy as jnp
from jax import lax
from jax.experimental import pallas as pl
from jax.experimental.pallas import tpu as pltpu
from jax.sharding import PartitionSpec as P

LEVELS = 16
GROUP = 16
OCTET = 8
LANES = 128
CHUNK = 256
NX, NZ, NY, NC = 4, 2, 4, 2
RANKS = NX * NZ * NY * NC
SEATS = NX * NY
STEPS = SEATS // 2
FRONT = 4
SEND = 8
MESH = pl.DeviceIdType.MESH


def kernel(bins_hbm, hess_hbm, thr_hbm, out_ref, bins_ref, hess_ref, thr_ref, prefix, column_ref, cols, wts, stage, inbox, mine, load_sem, send_sem, recv_sem, gather_send, gather_recv):
    words, width = bins_ref.shape
    tiles = words // LANES
    hess_load = pltpu.make_async_copy(hess_hbm, hess_ref, load_sem.at[tiles])
    hess_load.start()
    bins_loads = []
    for t in range(tiles):
        part = pl.ds(t * LANES, LANES)
        bins_loads.append(pltpu.make_async_copy(bins_hbm.at[part, :], bins_ref.at[part, :], load_sem.at[t]))
        bins_loads[t].start()
    thr_load = pltpu.make_async_copy(thr_hbm, thr_ref, load_sem.at[tiles + 1])
    thr_load.start()
    me = lax.axis_index("rows")
    x, z, y, core = me // (NZ * NY * NC), me // (NY * NC) % NZ, me // NC % NY, me % NC
    owner = (core == NC - 1) & (z == 0)

    def device(px, pz, py, pc):
        return ((px * NZ + pz) * NY + py) * NC + pc

    barrier = pltpu.get_barrier_semaphore()

    @pl.when(owner)
    def _():
        for step in range(1, RANKS):
            pl.semaphore_signal(barrier, inc=1, device_id={"rows": (me + step) % RANKS}, device_id_type=MESH)

    src = lax.broadcasted_iota(jnp.int32, (LANES, LANES), 0)
    dst = lax.broadcasted_iota(jnp.int32, (LANES, LANES), 1)
    gap = dst - src
    same = jnp.bitwise_and(gap, OCTET - 1) == 0
    prefix[:, :LANES] = jnp.where(jnp.logical_and(same, gap > 0), 1.0, 0.0).astype(jnp.bfloat16)
    prefix[:, LANES:] = jnp.where(same, 1.0, 0.0).astype(jnp.bfloat16)

    quarter = LANES // 4
    order = jnp.where(src == 4 * (dst % quarter) + dst // quarter, 1.0, 0.0).astype(jnp.bfloat16)
    lane = lax.broadcasted_iota(jnp.int32, (2 * tiles, LANES), 1) // quarter
    hess_load.wait()
    flat = jnp.concatenate([hess_ref[pl.ds(j, tiles, stride=4), :] for j in range(4)], axis=0)
    left_factor = jnp.ones_like(flat)
    miss = jnp.abs(flat - flat.astype(jnp.bfloat16).astype(jnp.float32))
    for j in range(1, 128, 2):
        factor = 1.0 + j / 128.0
        other = (flat * (1.0 / factor)).astype(jnp.bfloat16).astype(jnp.float32)
        away = jnp.abs(flat - other * factor)
        left_factor = jnp.where(away < miss, factor, left_factor)
        miss = jnp.minimum(miss, away)
        if j == 63:
            for t in range(tiles // 2):
                bins_loads[t].wait()
            for t in range(tiles // 2):
                cols[:, t * LANES : (t + 1) * LANES] = bins_ref[t * LANES : (t + 1) * LANES, :].T
    right_factor = flat / left_factor
    for t in range(tiles // 2, tiles):
        bins_loads[t].wait()
    thr_load.wait()
    for t in range(tiles // 2, tiles):
        cols[:, t * LANES : (t + 1) * LANES] = bins_ref[t * LANES : (t + 1) * LANES, :].T
    column_ref[...] = jnp.broadcast_to(thr_ref[...], (LANES, thr_ref.shape[1])).T
    pieces = jnp.concatenate([x[j * tiles : (j + 1) * tiles] for j in range(4) for x in (left_factor, right_factor)], axis=0)
    moved = jnp.dot(pieces.astype(jnp.bfloat16), order, preferred_element_type=jnp.float32)
    for k in range(4):
        plane = None
        for j in range(4):
            block = moved[2 * tiles * j : 2 * tiles * (j + 1)]
            if j != k:
                block = pltpu.roll(block, (quarter * (j - k)) % LANES, 1)
            plane = block if plane is None else jnp.where(lane == j, block, plane)
        for piece in range(2):
            for t in range(tiles):
                line = plane[piece * tiles + t : piece * tiles + t + 1]
                wts[piece, k, :, t * LANES : (t + 1) * LANES] = jnp.broadcast_to(line, (GROUP, LANES)).astype(jnp.bfloat16)

    sub = lax.broadcasted_iota(jnp.int32, (OCTET, LANES), 0)
    diagonal = sub == lax.broadcasted_iota(jnp.int32, (OCTET, LANES), 1) % OCTET

    def gather_rows(tiles8):
        low4, low2, low1 = sub < 4, sub % 4 < 2, sub % 2 < 1
        four = []
        for a in range(4):
            p, q = tiles8[a], tiles8[a + 4]
            four.append(jnp.where(low4, p, q) + pltpu.roll(jnp.where(low4, q, p), 4, 0))
        two = []
        for a in range(2):
            p, q = four[a], four[a + 2]
            two.append(jnp.where(low2, p, q) + jnp.where(low2, pltpu.roll(p, 6, 0), pltpu.roll(q, 2, 0)))
        p, q = two
        return jnp.where(low1, p, q) + jnp.where(low1, pltpu.roll(p, 7, 0), pltpu.roll(q, 1, 0))

    def products(group, first, last, sums):
        base = pl.multiple_of(group * GROUP, GROUP)
        zero = jnp.zeros((GROUP, CHUNK), jnp.bfloat16)
        upper = lax.broadcasted_iota(jnp.int32, (GROUP, CHUNK), 0) // OCTET
        for index in range(first, last):
            c, k = index // 4, index % 4
            part = cols[pl.ds(base, GROUP), c * CHUNK : (c + 1) * CHUNK]
            high = jnp.bitwise_and(jnp.right_shift(part, 8 * k + 4), 15).astype(jnp.float32).astype(jnp.bfloat16)
            low = jnp.bitwise_and(jnp.right_shift(part, 8 * k), 15)
            w0 = wts[0, k, :, c * CHUNK : (c + 1) * CHUNK]
            w1 = wts[1, k, :, c * CHUNK : (c + 1) * CHUNK]
            left = jnp.concatenate([jnp.where(high == jnp.bfloat16(h), w0, zero) for h in range(LEVELS)], axis=0)
            rights = []
            for o in range(2):
                eight = low[o * OCTET : (o + 1) * OCTET]
                pair = (jnp.concatenate([eight, eight], axis=0) - upper).astype(jnp.float32).astype(jnp.bfloat16)
                rights += [jnp.where(pair == jnp.bfloat16(l), w1, zero) for l in range(0, LEVELS, 2)]
            right = jnp.concatenate(rights, axis=0)
            part_sum = lax.dot_general(left, right, (((1,), (1,)), ((), ())), preferred_element_type=jnp.float32)
            side = index % 2
            sums[side] = part_sum if sums[side] is None else sums[side] + part_sum

    def extract(sums):
        blocks = []
        for o in range(2):
            cut = slice(o * LANES, (o + 1) * LANES)
            rows = []
            for h in range(LEVELS):
                pick = slice(h * GROUP + o * OCTET, h * GROUP + (o + 1) * OCTET)
                rows.append(jnp.where(diagonal, sums[0][pick, cut], 0.0) + jnp.where(diagonal, sums[1][pick, cut], 0.0))
            blocks.append(jnp.concatenate([gather_rows(rows[:8]), gather_rows(rows[8:])], axis=0))
        return blocks

    place_x, place_y = (x + 1) % NX, (y + 1) % NY

    def group_of(step):
        block_x = (place_x // 2 + (1 if step < 4 else 0)) % 2
        block_y = (place_y // 2 + (1 if step % 4 < 2 else 0)) % 2
        return 2 * block_x + (place_x + 1 - step % 2) % 2, block_y

    def outgoing(step, o):
        column, block_y = group_of(step)
        target = device((column + NX - 1) % NX, 0, (2 * block_y + o + NY - 1) % NY, NC - 1)
        return pltpu.make_async_remote_copy(
            src_ref=stage.at[step, o],
            dst_ref=inbox.at[step * OCTET + place_y % 2 * 4 + z * 2 + core],
            send_sem=send_sem.at[0],
            recv_sem=recv_sem.at[step // (STEPS - 1)],
            device_id={"rows": target},
            device_id_type=MESH,
        )

    pl.semaphore_wait(barrier, SEATS - owner.astype(jnp.int32))
    pieces_all = words // CHUNK * 4

    def keep(step, sums):
        for o, block in enumerate(extract(sums)):
            stage[step, o] = block

    def send(step):
        for o in range(2):
            if step < STEPS - 1:
                outgoing(step, o).start()
            else:

                own = owner & (place_y % 2 == o)

                @pl.when(own)
                def _():
                    inbox[step * OCTET + o * 4 + core] = stage[step, o]

                @pl.when(jnp.logical_not(own))
                def _():
                    outgoing(step, o).start()

    before_sums = None
    for step in range(STEPS):
        column, block_y = group_of(step)
        group = column * 2 + block_y
        sums = [None, None]
        products(group, 0, FRONT, sums)
        if step > 0:
            keep(step - 1, before_sums)
        products(group, FRONT, SEND, sums)
        if step > 0:
            send(step - 1)
        products(group, SEND, pieces_all, sums)
        before_sums = sums
    keep(STEPS - 1, before_sums)
    send(STEPS - 1)

    def spread(target):
        return pltpu.make_async_remote_copy(
            src_ref=mine,
            dst_ref=out_ref.at[pl.ds(here, OCTET), :],
            send_sem=gather_send.at[0],
            recv_sem=gather_recv.at[0],
            device_id={"rows": target},
            device_id_type=MESH,
        )

    def spread_owners():
        first = (NX - x) % NX * NY + (NY - y) % NY
        for k in range(SEATS - 1):
            shift = (first + k) % SEATS
            shift = shift + (1 - (shift + SEATS - 1) // SEATS) * ((first + SEATS - 1) % SEATS)
            yield spread(device((x + shift // NY) % NX, 0, (y + shift % NY) % NY, NC - 1))

    def spread_chip(px, py):
        for pz, pc in ((1, 1), (1, 0), (0, 0)):
            yield spread(device(px, pz, py, pc))

    def drain(ref, sem):
        return pltpu.make_async_copy(ref, ref, sem)

    here = pl.multiple_of((place_x * NY + place_y) * OCTET, OCTET)
    late = (0, 1, 2, 2)
    chips = sorted(((px, py) for px in range(NX) for py in range(NY)), key=lambda c: late[c[0]] + late[c[1]])

    @pl.when(owner)
    def _():
        drain(inbox.at[pl.ds(0, RANKS - OCTET)], recv_sem.at[0]).wait()
        sums = [None] * 4
        for s in range(RANKS - OCTET):
            sums[s % 4] = inbox[s] if sums[s % 4] is None else sums[s % 4] + inbox[s]
        drain(inbox.at[pl.ds(0, OCTET - 1)], recv_sem.at[1]).wait()
        for s in range(RANKS - OCTET, RANKS):
            sums[s % 4] = sums[s % 4] + inbox[s]
        total = (sums[0] + sums[1]) + (sums[2] + sums[3])

        p0 = total.astype(jnp.bfloat16).astype(jnp.float32)
        p1 = (total - p0).astype(jnp.bfloat16).astype(jnp.float32)
        p2 = total - p0 - p1
        split = jnp.concatenate([p0, p1, p2], axis=0).astype(jnp.bfloat16)
        sums3 = jnp.dot(split, prefix[...], preferred_element_type=jnp.float32)
        joined = sums3[:LEVELS] + sums3[LEVELS : 2 * LEVELS] + sums3[2 * LEVELS :]
        inner, level = joined[:, :LANES], joined[:, LANES:]
        inv = 1.0 / (total + 1.0)
        whole = jnp.sum(level, axis=0, keepdims=True)
        target = column_ref[...] * whole
        run = jnp.zeros((1, LANES), jnp.float32)
        acc = jnp.zeros((thr_ref.shape[1], LANES), jnp.float32)
        for h in range(LEVELS):
            before = inner[h : h + 1] + run
            run = run + level[h : h + 1]
            ratio = (target - before) * inv[h : h + 1]
            acc = acc + jnp.clip(ratio, 0.0, 1.0)
        turned = acc.T
        cuts = turned[:OCTET]
        for j in range(1, LANES // OCTET):
            cuts = cuts + turned[j * OCTET : (j + 1) * OCTET]
        mine[...] = cuts
        owners = list(spread_owners())
        others = [copy for px, py in chips for copy in spread_chip(px, py)]
        copies = owners[:1] + others[:18] + owners[1:] + others[18:]
        for copy in copies:
            copy.start()
        out_ref[pl.ds(here, OCTET), :] = cuts
        drain(inbox.at[pl.ds(0, SEATS - 1)], send_sem.at[0]).wait()
        drain(out_ref.at[pl.ds(0, (SEATS - 1) * OCTET), :], gather_recv.at[0]).wait()
        for copy in copies:
            copy.wait_send()

    @pl.when(jnp.logical_not(owner))
    def _():
        drain(inbox.at[pl.ds(0, SEATS)], send_sem.at[0]).wait()
        drain(out_ref, gather_recv.at[0]).wait()


def solution(mesh):
    def local(bins, hessian, thresholds):
        words, width = bins.shape
        quantiles = thresholds.shape[0]
        return pl.pallas_call(
            kernel,
            out_shape=pltpu.VMEM((width, quantiles), jnp.float32),
            in_specs=[pl.BlockSpec(memory_space=pl.ANY)] * 3,
            out_specs=pl.BlockSpec(memory_space=pltpu.VMEM),
            scratch_shapes=[
                pltpu.VMEM((words, width), jnp.int32),
                pltpu.VMEM((4 * words // LANES, LANES), jnp.float32),
                pltpu.VMEM((1, quantiles), jnp.float32),
                pltpu.VMEM((LANES, 2 * LANES), jnp.bfloat16),
                pltpu.VMEM((quantiles, LANES), jnp.float32),
                pltpu.VMEM((width, words), jnp.int32),
                pltpu.VMEM((2, 4, GROUP, words), jnp.bfloat16),
                pltpu.VMEM((STEPS, 2, LEVELS, LANES), jnp.float32),
                pltpu.VMEM((RANKS, LEVELS, LANES), jnp.float32),
                pltpu.VMEM((OCTET, quantiles), jnp.float32),
                pltpu.SemaphoreType.DMA((words // LANES + 2,)),
                pltpu.SemaphoreType.DMA((1,)),
                pltpu.SemaphoreType.DMA((2,)),
                pltpu.SemaphoreType.DMA((1,)),
                pltpu.SemaphoreType.DMA((1,)),
            ],
            compiler_params=pltpu.CompilerParams(collective_id=0, has_side_effects=True),
        )(bins, hessian.reshape(-1, LANES), thresholds.reshape(1, -1))

    in_specs = (P("rows", "feat"), P("rows"), P())
    return jax.shard_map(local, mesh=mesh, in_specs=in_specs, out_specs=P("feat", None), check_vma=False)
```

```python
import jax
import jax.numpy as jnp
from jax import lax
from jax.experimental import pallas as pl
from jax.experimental.pallas import tpu as pltpu
from jax.sharding import PartitionSpec as P

LEVELS = 16
GROUP = 16
OCTET = 8
LANES = 128
CHUNK = 256
NX, NZ, NY, NC = 4, 2, 4, 2
RANKS = NX * NZ * NY * NC
SEATS = NX * NY
STEPS = 4
FRONT = 4
SEND = 8
MEET = 8
SLOTS = STEPS * OCTET
MESH = pl.DeviceIdType.MESH


def mod(value, size):
    return lax.rem(value, jnp.int32(size)) if isinstance(value, jax.Array) else value % size


def div(value, size):
    return lax.div(value, jnp.int32(size)) if isinstance(value, jax.Array) else value // size


def kernel(bins_hbm, hess_hbm, thr_hbm, out_ref, bins_ref, hess_ref, thr_ref, prefix, column_ref, cols, wts, lines, other_cols, other_wts, other_lines, partial, stage, inbox, mine, load_sem, swap_send, swap_recv, send_sem, recv_sem, gather_send, gather_recv, hello, go):
    words, width = bins_ref.shape
    tiles = words // LANES
    hess_load = pltpu.make_async_copy(hess_hbm, hess_ref, load_sem.at[tiles])
    hess_load.start()
    bins_loads = []
    for t in range(tiles):
        part = pl.ds(t * LANES, LANES)
        bins_loads.append(pltpu.make_async_copy(bins_hbm.at[part, :], bins_ref.at[part, :], load_sem.at[t]))
        bins_loads[t].start()
    thr_load = pltpu.make_async_copy(thr_hbm, thr_ref, load_sem.at[tiles + 1])
    thr_load.start()
    me = lax.axis_index("rows")
    x, z, y, core = div(me, NZ * NY * NC), mod(div(me, NY * NC), NZ), mod(div(me, NC), NY), mod(me, NC)
    owner = (core == NC - 1) & (z == 0)

    def device(px, pz, py, pc):
        return ((px * NZ + pz) * NY + py) * NC + pc

    partner = device(x, z, y, 1 - core)
    barrier = pltpu.get_barrier_semaphore()

    @pl.when(core == 1)
    def _():
        pl.semaphore_signal(barrier, inc=1, device_id={"rows": partner}, device_id_type=MESH)

    @pl.when(owner)
    def _():
        for step in range(NC, RANKS, NC):
            pl.semaphore_signal(barrier, inc=1, device_id={"rows": mod(me + step, RANKS)}, device_id_type=MESH)

    @pl.when(core == 0)
    def _():
        pl.semaphore_wait(barrier, 1)
        pl.semaphore_signal(hello, inc=1, device_id={"rows": partner}, device_id_type=MESH)

    src = lax.broadcasted_iota(jnp.int32, (LANES, LANES), 0)
    dst = lax.broadcasted_iota(jnp.int32, (LANES, LANES), 1)
    gap = dst - src
    same = jnp.bitwise_and(gap, OCTET - 1) == 0
    prefix[:, :LANES] = jnp.where(jnp.logical_and(same, gap > 0), 1.0, 0.0).astype(jnp.bfloat16)
    prefix[:, LANES:] = jnp.where(same, 1.0, 0.0).astype(jnp.bfloat16)

    quarter = LANES // 4
    order = jnp.where(src == 4 * (dst % quarter) + dst // quarter, 1.0, 0.0).astype(jnp.bfloat16)
    lane = lax.broadcasted_iota(jnp.int32, (2 * tiles, LANES), 1) // quarter
    hess_load.wait()
    flat = jnp.concatenate([hess_ref[pl.ds(j, tiles, stride=4), :] for j in range(4)], axis=0)
    left_factor = jnp.ones_like(flat)
    miss = jnp.abs(flat - flat.astype(jnp.bfloat16).astype(jnp.float32))
    for j in range(1, 128, 2):
        factor = 1.0 + j / 128.0
        other = (flat * (1.0 / factor)).astype(jnp.bfloat16).astype(jnp.float32)
        away = jnp.abs(flat - other * factor)
        left_factor = jnp.where(away < miss, factor, left_factor)
        miss = jnp.minimum(miss, away)
        if j == 63:
            for t in range(tiles // 2):
                bins_loads[t].wait()
            for t in range(tiles // 2):
                cols[:, t * LANES : (t + 1) * LANES] = bins_ref[t * LANES : (t + 1) * LANES, :].T
    right_factor = flat / left_factor
    for t in range(tiles // 2, tiles):
        bins_loads[t].wait()
    thr_load.wait()
    for t in range(tiles // 2, tiles):
        cols[:, t * LANES : (t + 1) * LANES] = bins_ref[t * LANES : (t + 1) * LANES, :].T
    column_ref[...] = jnp.broadcast_to(thr_ref[...], (LANES, thr_ref.shape[1])).T
    pieces = jnp.concatenate([x[j * tiles : (j + 1) * tiles] for j in range(4) for x in (left_factor, right_factor)], axis=0)
    moved = jnp.dot(pieces.astype(jnp.bfloat16), order, preferred_element_type=jnp.float32)
    for k in range(4):
        plane = None
        for j in range(4):
            block = moved[2 * tiles * j : 2 * tiles * (j + 1)]
            if j != k:
                block = pltpu.roll(block, (quarter * (j - k)) % LANES, 1)
            plane = block if plane is None else jnp.where(lane == j, block, plane)
        lines[k] = plane

    def widen(target, source):
        for k in range(4):
            plane = source[k]
            for piece in range(2):
                for t in range(tiles):
                    line = plane[piece * tiles + t : piece * tiles + t + 1]
                    target[piece, k, :, t * LANES : (t + 1) * LANES] = jnp.broadcast_to(line, (GROUP, LANES)).astype(jnp.bfloat16)

    half = width // 4

    def swap(piece):
        if piece < 2:
            there = pl.multiple_of(piece * 2 * half + (1 - core) * half, half)
            source, target = cols.at[pl.ds(there, half), :], other_cols.at[pl.ds(piece * half, half), :]
        else:
            source, target = lines, other_lines
        return pltpu.make_async_remote_copy(
            src_ref=source,
            dst_ref=target,
            send_sem=swap_send.at[piece],
            recv_sem=swap_recv.at[piece],
            device_id={"rows": partner},
            device_id_type=MESH,
        )

    @pl.when(core == 1)
    def _():
        pl.semaphore_wait(hello, 1)

    for piece in (2, 0, 1):
        swap(piece).start()
    widen(wts, lines)

    sub = lax.broadcasted_iota(jnp.int32, (OCTET, LANES), 0)
    diagonal = sub == lax.broadcasted_iota(jnp.int32, (OCTET, LANES), 1) % OCTET

    def gather_rows(tiles8):
        low4, low2, low1 = sub < 4, sub % 4 < 2, sub % 2 < 1
        four = []
        for a in range(4):
            p, q = tiles8[a], tiles8[a + 4]
            four.append(jnp.where(low4, p, q) + pltpu.roll(jnp.where(low4, q, p), 4, 0))
        two = []
        for a in range(2):
            p, q = four[a], four[a + 2]
            two.append(jnp.where(low2, p, q) + jnp.where(low2, pltpu.roll(p, 6, 0), pltpu.roll(q, 2, 0)))
        p, q = two
        return jnp.where(low1, p, q) + jnp.where(low1, pltpu.roll(p, 7, 0), pltpu.roll(q, 1, 0))

    def products(columns, weights, base, first, last, sums):
        zero = jnp.zeros((GROUP, CHUNK), jnp.bfloat16)
        upper = lax.broadcasted_iota(jnp.int32, (GROUP, CHUNK), 0) // OCTET
        for index in range(first, last):
            c, k = index // 4, index % 4
            part = columns[pl.ds(base, GROUP), c * CHUNK : (c + 1) * CHUNK]
            high = jnp.bitwise_and(jnp.right_shift(part, 8 * k + 4), 15).astype(jnp.float32).astype(jnp.bfloat16)
            low = jnp.bitwise_and(jnp.right_shift(part, 8 * k), 15)
            w0 = weights[0, k, :, c * CHUNK : (c + 1) * CHUNK]
            w1 = weights[1, k, :, c * CHUNK : (c + 1) * CHUNK]
            left = jnp.concatenate([jnp.where(high == jnp.bfloat16(h), w0, zero) for h in range(LEVELS)], axis=0)
            rights = []
            for o in range(2):
                eight = low[o * OCTET : (o + 1) * OCTET]
                pair = (jnp.concatenate([eight, eight], axis=0) - upper).astype(jnp.float32).astype(jnp.bfloat16)
                rights += [jnp.where(pair == jnp.bfloat16(l), w1, zero) for l in range(0, LEVELS, 2)]
            right = jnp.concatenate(rights, axis=0)
            part_sum = lax.dot_general(left, right, (((1,), (1,)), ((), ())), preferred_element_type=jnp.float32)
            side = index % 2
            sums[side] = part_sum if sums[side] is None else sums[side] + part_sum

    def extract(sums):
        blocks = []
        for o in range(2):
            cut = slice(o * LANES, (o + 1) * LANES)
            rows = []
            for h in range(LEVELS):
                pick = slice(h * GROUP + o * OCTET, h * GROUP + (o + 1) * OCTET)
                rows.append(jnp.where(diagonal, sums[0][pick, cut], 0.0) + jnp.where(diagonal, sums[1][pick, cut], 0.0))
            blocks.append([gather_rows(rows[:8]), gather_rows(rows[8:])])
        return blocks

    place_x, place_y = mod(x + 1, NX), mod(y + 1, NY)

    def block_of(step):
        return mod(div(place_x, 2) + (1 if step < 2 else 0), 2), mod(div(place_y, 2) + (1 if step % 2 == 0 else 0), 2)

    def outgoing(step, o):
        block_x, block_y = block_of(step)
        target = device(mod(2 * block_x + core + NX - 1, NX), 0, mod(2 * block_y + o + NY - 1, NY), NC - 1)
        return pltpu.make_async_remote_copy(
            src_ref=stage.at[step, o],
            dst_ref=inbox.at[pl.ds(2 * (step * OCTET + mod(place_x, 2) * 4 + mod(place_y, 2) * 2 + z), 2)],
            send_sem=send_sem.at[0],
            recv_sem=recv_sem.at[step // (STEPS - 1)],
            device_id={"rows": target},
            device_id_type=MESH,
        )

    pieces_all = words // CHUNK * 4
    keeps = owner & (mod(place_x, 2) == core)

    def keep(step, theirs, alone, sums):
        for o, block in enumerate(extract(sums)):
            for part in range(2):
                if not theirs:
                    partial[step, o, part] = block[part]
                else:
                    stage[step, o, part] = block[part] if alone else block[part] + partial[step, o, part]

    def send(step):
        for o in range(2):
            if step < STEPS - 1:
                outgoing(step, o).start()
            else:
                own = keeps & (mod(place_y, 2) == o)

                @pl.when(own)
                def _():
                    inbox[pl.ds(2 * (step * OCTET + mod(place_x, 2) * 4 + o * 2), 2)] = stage[step, o]

                @pl.when(jnp.logical_not(own))
                def _():
                    outgoing(step, o).start()

    def span(step, theirs, first, last, sums):
        block_x, block_y = block_of(step)
        if theirs:
            base = pl.multiple_of(block_x * half + block_y * GROUP, GROUP)
            products(other_cols, other_wts, base, first, last, sums)
        else:
            base = pl.multiple_of((2 * block_x + core) * half + block_y * GROUP, GROUP)
            products(cols, wts, base, first, last, sums)

    parts = [(step, theirs) for theirs in (False, True) for step in range(STEPS - 1)] + [(STEPS - 1, False)]
    last = None
    for index, (step, theirs) in enumerate(parts):
        sums = [None, None]
        span(step, theirs, 0, FRONT, sums)
        if last is not None:
            keep(*last)
        span(step, theirs, FRONT, SEND, sums)
        if last is not None and last[1]:
            if last[0] == 0:
                @pl.when(core == 1)
                def _():
                    pl.semaphore_wait(barrier, SEATS - owner.astype(jnp.int32))
                    pl.semaphore_signal(go, inc=1, device_id={"rows": partner}, device_id_type=MESH)

                @pl.when(core == 0)
                def _():
                    pl.semaphore_wait(go, 1)

            send(last[0])
        if index == STEPS - 2:
            span(step, theirs, SEND, MEET, sums)
            for piece in range(3):
                swap(piece).wait()
            widen(other_wts, other_lines)
            span(step, theirs, MEET, pieces_all, sums)
        else:
            span(step, theirs, SEND, pieces_all, sums)
        last = step, theirs, False, sums
    span(STEPS - 1, True, 0, pieces_all, sums)
    keep(STEPS - 1, True, True, sums)
    send(STEPS - 1)

    def spread(target):
        return pltpu.make_async_remote_copy(
            src_ref=mine,
            dst_ref=out_ref.at[pl.ds(here, OCTET), :],
            send_sem=gather_send.at[0],
            recv_sem=gather_recv.at[0],
            device_id={"rows": target},
            device_id_type=MESH,
        )

    def spread_owners():
        first = mod(NX - x, NX) * NY + mod(NY - y, NY)
        for k in range(SEATS - 1):
            shift = mod(first + k, SEATS)
            shift = shift + (1 - div(shift + SEATS - 1, SEATS)) * mod(first + SEATS - 1, SEATS)
            yield spread(device(mod(x + div(shift, NY), NX), 0, mod(y + mod(shift, NY), NY), NC - 1))

    def spread_chip(px, py):
        for pz, pc in ((1, 1), (1, 0), (0, 0)):
            yield spread(device(px, pz, py, pc))

    def drain(ref, sem):
        return pltpu.make_async_copy(ref, ref, sem)

    here = pl.multiple_of((place_x * NY + place_y) * OCTET, OCTET)
    late = (0, 1, 2, 2)
    chips = sorted(((px, py) for px in range(NX) for py in range(NY)), key=lambda c: late[c[0]] + late[c[1]])

    @pl.when(keeps)
    def _():
        drain(inbox.at[pl.ds(0, 2 * (2 * STEPS - 1))], send_sem.at[0]).wait()

    @pl.when(jnp.logical_not(keeps))
    def _():
        drain(inbox.at[pl.ds(0, 4 * STEPS)], send_sem.at[0]).wait()

    @pl.when(owner)
    def _():
        drain(inbox.at[pl.ds(0, 2 * (SLOTS - OCTET))], recv_sem.at[0]).wait()
        sums = [None] * 4
        for s in range(2 * (SLOTS - OCTET)):
            sums[s % 4] = inbox[s] if sums[s % 4] is None else sums[s % 4] + inbox[s]

        @pl.when(keeps)
        def _():
            drain(inbox.at[pl.ds(0, 2 * (OCTET - 1))], recv_sem.at[1]).wait()

        @pl.when(jnp.logical_not(keeps))
        def _():
            drain(inbox.at[pl.ds(0, 2 * OCTET)], recv_sem.at[1]).wait()

        for s in range(2 * (SLOTS - OCTET), 2 * SLOTS):
            sums[s % 4] = sums[s % 4] + inbox[s]
        total = jnp.concatenate([sums[0] + sums[2], sums[1] + sums[3]], axis=0)

        p0 = total.astype(jnp.bfloat16).astype(jnp.float32)
        p1 = (total - p0).astype(jnp.bfloat16).astype(jnp.float32)
        p2 = total - p0 - p1
        split = jnp.concatenate([p0, p1, p2], axis=0).astype(jnp.bfloat16)
        sums3 = jnp.dot(split, prefix[...], preferred_element_type=jnp.float32)
        joined = sums3[:LEVELS] + sums3[LEVELS : 2 * LEVELS] + sums3[2 * LEVELS :]
        inner, level = joined[:, :LANES], joined[:, LANES:]
        inv = 1.0 / (total + 1.0)
        whole = jnp.sum(level, axis=0, keepdims=True)
        target = column_ref[...] * whole
        run = jnp.zeros((1, LANES), jnp.float32)
        acc = jnp.zeros((thr_ref.shape[1], LANES), jnp.float32)
        for h in range(LEVELS):
            before = inner[h : h + 1] + run
            run = run + level[h : h + 1]
            ratio = (target - before) * inv[h : h + 1]
            acc = acc + jnp.clip(ratio, 0.0, 1.0)
        turned = acc.T
        cuts = turned[:OCTET]
        for j in range(1, LANES // OCTET):
            cuts = cuts + turned[j * OCTET : (j + 1) * OCTET]
        mine[...] = cuts
        owners = list(spread_owners())
        others = [copy for px, py in chips for copy in spread_chip(px, py)]
        copies = owners[:1] + others[:18] + owners[1:] + others[18:]
        for copy in copies:
            copy.start()
        out_ref[pl.ds(here, OCTET), :] = cuts
        drain(inbox.at[pl.ds(0, RANKS - 1)], gather_send.at[0]).wait()
        drain(out_ref.at[pl.ds(0, (SEATS - 1) * OCTET), :], gather_recv.at[0]).wait()

    @pl.when(jnp.logical_not(owner))
    def _():
        drain(out_ref, gather_recv.at[0]).wait()


def solution(mesh):
    def local(bins, hessian, thresholds):
        words, width = bins.shape
        quantiles = thresholds.shape[0]
        return pl.pallas_call(
            kernel,
            out_shape=pltpu.VMEM((width, quantiles), jnp.float32),
            in_specs=[pl.BlockSpec(memory_space=pl.ANY)] * 3,
            out_specs=pl.BlockSpec(memory_space=pltpu.VMEM),
            scratch_shapes=[
                pltpu.VMEM((words, width), jnp.int32),
                pltpu.VMEM((4 * words // LANES, LANES), jnp.float32),
                pltpu.VMEM((1, quantiles), jnp.float32),
                pltpu.VMEM((LANES, 2 * LANES), jnp.bfloat16),
                pltpu.VMEM((quantiles, LANES), jnp.float32),
                pltpu.VMEM((width, words), jnp.int32),
                pltpu.VMEM((2, 4, GROUP, words), jnp.bfloat16),
                pltpu.VMEM((4, 2 * words // LANES, LANES), jnp.float32),
                pltpu.VMEM((width // 2, words), jnp.int32),
                pltpu.VMEM((2, 4, GROUP, words), jnp.bfloat16),
                pltpu.VMEM((4, 2 * words // LANES, LANES), jnp.float32),
                pltpu.VMEM((STEPS, 2, 2, OCTET, LANES), jnp.float32),
                pltpu.VMEM((STEPS, 2, 2, OCTET, LANES), jnp.float32),
                pltpu.VMEM((2 * SLOTS, OCTET, LANES), jnp.float32),
                pltpu.VMEM((OCTET, quantiles), jnp.float32),
                pltpu.SemaphoreType.DMA((words // LANES + 2,)),
                pltpu.SemaphoreType.DMA((3,)),
                pltpu.SemaphoreType.DMA((3,)),
                pltpu.SemaphoreType.DMA((1,)),
                pltpu.SemaphoreType.DMA((2,)),
                pltpu.SemaphoreType.DMA((1,)),
                pltpu.SemaphoreType.DMA((1,)),
                pltpu.SemaphoreType.REGULAR,
                pltpu.SemaphoreType.REGULAR,
            ],
            compiler_params=pltpu.CompilerParams(collective_id=0, has_side_effects=True),
        )(bins, hessian.reshape(-1, LANES), thresholds.reshape(1, -1))

    in_specs = (P("rows", "feat"), P("rows"), P())
    return jax.shard_map(local, mesh=mesh, in_specs=in_specs, out_specs=P("feat", None), check_vma=False)
```

```python
import jax
import jax.numpy as jnp
from jax import lax
from jax.experimental import pallas as pl
from jax.experimental.pallas import tpu as pltpu
from jax.sharding import PartitionSpec as P

LEVELS = 16
GROUP = 16
OCTET = 8
LANES = 128
CHUNK = 256
NX, NZ, NY, NC = 4, 2, 4, 2
RANKS = NX * NZ * NY * NC
SEATS = NX * NY
STEPS = 4
FRONT = 4
SEND = 8
MEET = 8
SLOTS = STEPS * OCTET
MESH = pl.DeviceIdType.MESH


def mod(value, size):
    return lax.rem(value, jnp.int32(size)) if isinstance(value, jax.Array) else value % size


def div(value, size):
    return lax.div(value, jnp.int32(size)) if isinstance(value, jax.Array) else value // size


def kernel(bins_hbm, hess_hbm, thr_hbm, out_ref, bins_ref, hess_ref, thr_ref, prefix, column_ref, cols, wts, lines, other_cols, other_wts, other_lines, partial, stage, inbox, mine, load_sem, swap_send, swap_recv, send_sem, recv_sem, gather_send, gather_recv, hello, go):
    words, width = bins_ref.shape
    tiles = words // LANES
    hess_load = pltpu.make_async_copy(hess_hbm, hess_ref, load_sem.at[tiles])
    hess_load.start()
    bins_loads = []
    for t in range(tiles):
        part = pl.ds(t * LANES, LANES)
        bins_loads.append(pltpu.make_async_copy(bins_hbm.at[part, :], bins_ref.at[part, :], load_sem.at[t]))
        bins_loads[t].start()
    thr_load = pltpu.make_async_copy(thr_hbm, thr_ref, load_sem.at[tiles + 1])
    thr_load.start()
    me = lax.axis_index("rows")
    x, z, y, core = div(me, NZ * NY * NC), mod(div(me, NY * NC), NZ), mod(div(me, NC), NY), mod(me, NC)
    owner = (core == NC - 1) & (z == 0)

    def device(px, pz, py, pc):
        return ((px * NZ + pz) * NY + py) * NC + pc

    partner = device(x, z, y, 1 - core)
    barrier = pltpu.get_barrier_semaphore()

    @pl.when(core == 1)
    def _():
        pl.semaphore_signal(barrier, inc=1, device_id={"rows": partner}, device_id_type=MESH)

    @pl.when(owner)
    def _():
        for step in range(NC, RANKS, NC):
            pl.semaphore_signal(barrier, inc=1, device_id={"rows": mod(me + step, RANKS)}, device_id_type=MESH)

    @pl.when(core == 0)
    def _():
        pl.semaphore_wait(barrier, 1)
        pl.semaphore_signal(hello, inc=1, device_id={"rows": partner}, device_id_type=MESH)

    src = lax.broadcasted_iota(jnp.int32, (LANES, LANES), 0)
    dst = lax.broadcasted_iota(jnp.int32, (LANES, LANES), 1)
    gap = dst - src
    same = jnp.bitwise_and(gap, OCTET - 1) == 0
    prefix[:, :LANES] = jnp.where(jnp.logical_and(same, gap > 0), 1.0, 0.0).astype(jnp.bfloat16)
    prefix[:, LANES:] = jnp.where(same, 1.0, 0.0).astype(jnp.bfloat16)

    quarter = LANES // 4
    order = jnp.where(src == 4 * (dst % quarter) + dst // quarter, 1.0, 0.0).astype(jnp.bfloat16)
    lane = lax.broadcasted_iota(jnp.int32, (2 * tiles, LANES), 1) // quarter
    hess_load.wait()
    flat = jnp.concatenate([hess_ref[pl.ds(j, tiles, stride=4), :] for j in range(4)], axis=0)
    left_factor = jnp.ones_like(flat)
    miss = jnp.abs(flat - flat.astype(jnp.bfloat16).astype(jnp.float32))
    for j in range(1, 128, 2):
        factor = 1.0 + j / 128.0
        other = (flat * (1.0 / factor)).astype(jnp.bfloat16).astype(jnp.float32)
        away = jnp.abs(flat - other * factor)
        left_factor = jnp.where(away < miss, factor, left_factor)
        miss = jnp.minimum(miss, away)
        if j == 63:
            for t in range(tiles // 2):
                bins_loads[t].wait()
            for t in range(tiles // 2):
                cols[:, t * LANES : (t + 1) * LANES] = bins_ref[t * LANES : (t + 1) * LANES, :].T
    right_factor = flat / left_factor
    for t in range(tiles // 2, tiles):
        bins_loads[t].wait()
    thr_load.wait()
    for t in range(tiles // 2, tiles):
        cols[:, t * LANES : (t + 1) * LANES] = bins_ref[t * LANES : (t + 1) * LANES, :].T
    column_ref[...] = jnp.broadcast_to(thr_ref[...], (LANES, thr_ref.shape[1])).T
    pieces = jnp.concatenate([x[j * tiles : (j + 1) * tiles] for j in range(4) for x in (left_factor, right_factor)], axis=0)
    moved = jnp.dot(pieces.astype(jnp.bfloat16), order, preferred_element_type=jnp.float32)
    for k in range(4):
        plane = None
        for j in range(4):
            block = moved[2 * tiles * j : 2 * tiles * (j + 1)]
            if j != k:
                block = pltpu.roll(block, (quarter * (j - k)) % LANES, 1)
            plane = block if plane is None else jnp.where(lane == j, block, plane)
        lines[k] = plane

    def widen(target, source):
        for k in range(4):
            plane = source[k]
            for piece in range(2):
                for t in range(tiles):
                    line = plane[piece * tiles + t : piece * tiles + t + 1]
                    target[piece, k, :, t * LANES : (t + 1) * LANES] = jnp.broadcast_to(line, (GROUP, LANES)).astype(jnp.bfloat16)

    half = width // 4

    def swap(piece):
        if piece < 2:
            there = pl.multiple_of(piece * 2 * half + (1 - core) * half, half)
            source, target = cols.at[pl.ds(there, half), :], other_cols.at[pl.ds(piece * half, half), :]
        else:
            source, target = lines, other_lines
        return pltpu.make_async_remote_copy(
            src_ref=source,
            dst_ref=target,
            send_sem=swap_send.at[piece],
            recv_sem=swap_recv.at[piece],
            device_id={"rows": partner},
            device_id_type=MESH,
        )

    @pl.when(core == 1)
    def _():
        pl.semaphore_wait(hello, 1)

    for piece in (2, 0, 1):
        swap(piece).start()
    widen(wts, lines)

    sub = lax.broadcasted_iota(jnp.int32, (OCTET, LANES), 0)
    diagonal = sub == lax.broadcasted_iota(jnp.int32, (OCTET, LANES), 1) % OCTET

    def gather_rows(tiles8):
        low4, low2, low1 = sub < 4, sub % 4 < 2, sub % 2 < 1
        four = []
        for a in range(4):
            p, q = tiles8[a], tiles8[a + 4]
            four.append(jnp.where(low4, p, q) + pltpu.roll(jnp.where(low4, q, p), 4, 0))
        two = []
        for a in range(2):
            p, q = four[a], four[a + 2]
            two.append(jnp.where(low2, p, q) + jnp.where(low2, pltpu.roll(p, 6, 0), pltpu.roll(q, 2, 0)))
        p, q = two
        return jnp.where(low1, p, q) + jnp.where(low1, pltpu.roll(p, 7, 0), pltpu.roll(q, 1, 0))

    def products(columns, weights, base, first, last, sums):
        zero = jnp.zeros((GROUP, CHUNK), jnp.bfloat16)
        upper = lax.broadcasted_iota(jnp.int32, (GROUP, CHUNK), 0) // OCTET
        for index in range(first, last):
            c, k = index // 4, index % 4
            part = columns[pl.ds(base, GROUP), c * CHUNK : (c + 1) * CHUNK]
            high = jnp.bitwise_and(jnp.right_shift(part, 8 * k + 4), 15).astype(jnp.float32).astype(jnp.bfloat16)
            low = jnp.bitwise_and(jnp.right_shift(part, 8 * k), 15)
            w0 = weights[0, k, :, c * CHUNK : (c + 1) * CHUNK]
            w1 = weights[1, k, :, c * CHUNK : (c + 1) * CHUNK]
            left = jnp.concatenate([jnp.where(high == jnp.bfloat16(h), w0, zero) for h in range(LEVELS)], axis=0)
            rights = []
            for o in range(2):
                eight = low[o * OCTET : (o + 1) * OCTET]
                pair = (jnp.concatenate([eight, eight], axis=0) - upper).astype(jnp.float32).astype(jnp.bfloat16)
                rights += [jnp.where(pair == jnp.bfloat16(l), w1, zero) for l in range(0, LEVELS, 2)]
            right = jnp.concatenate(rights, axis=0)
            part_sum = lax.dot_general(left, right, (((1,), (1,)), ((), ())), preferred_element_type=jnp.float32)
            side = index % 2
            sums[side] = part_sum if sums[side] is None else sums[side] + part_sum

    def extract(sums):
        blocks = []
        for o in range(2):
            cut = slice(o * LANES, (o + 1) * LANES)
            rows = []
            for h in range(LEVELS):
                pick = slice(h * GROUP + o * OCTET, h * GROUP + (o + 1) * OCTET)
                rows.append(jnp.where(diagonal, sums[0][pick, cut], 0.0) + jnp.where(diagonal, sums[1][pick, cut], 0.0))
            blocks.append([gather_rows(rows[:8]), gather_rows(rows[8:])])
        return blocks

    place_x, place_y = mod(x + 1, NX), mod(y + 1, NY)

    def block_of(step):
        return mod(div(place_x, 2) + (1 if step < 2 else 0), 2), mod(div(place_y, 2) + (1 if step % 2 == 0 else 0), 2)

    def outgoing(step, o):
        block_x, block_y = block_of(step)
        target = device(mod(2 * block_x + core + NX - 1, NX), 0, mod(2 * block_y + o + NY - 1, NY), NC - 1)
        return pltpu.make_async_remote_copy(
            src_ref=stage.at[step, o],
            dst_ref=inbox.at[pl.ds(2 * (step * OCTET + mod(place_x, 2) * 4 + mod(place_y, 2) * 2 + z), 2)],
            send_sem=send_sem.at[0],
            recv_sem=recv_sem.at[step // (STEPS - 1)],
            device_id={"rows": target},
            device_id_type=MESH,
        )

    pieces_all = words // CHUNK * 4
    keeps = owner & (mod(place_x, 2) == core)

    def keep(step, theirs, alone, sums):
        for o, block in enumerate(extract(sums)):
            for part in range(2):
                if not theirs:
                    partial[step, o, part] = block[part]
                else:
                    stage[step, o, part] = block[part] if alone else block[part] + partial[step, o, part]

    def send(step):
        for o in range(2):
            if step < STEPS - 1:
                outgoing(step, o).start()
            else:
                own = keeps & (mod(place_y, 2) == o)

                @pl.when(own)
                def _():
                    inbox[pl.ds(2 * (step * OCTET + mod(place_x, 2) * 4 + o * 2), 2)] = stage[step, o]

                @pl.when(jnp.logical_not(own))
                def _():
                    outgoing(step, o).start()

    def span(step, theirs, first, last, sums):
        block_x, block_y = block_of(step)
        if theirs:
            base = pl.multiple_of(block_x * half + block_y * GROUP, GROUP)
            products(other_cols, other_wts, base, first, last, sums)
        else:
            base = pl.multiple_of((2 * block_x + core) * half + block_y * GROUP, GROUP)
            products(cols, wts, base, first, last, sums)

    parts = [(step, theirs) for theirs in (False, True) for step in range(STEPS - 1)] + [(STEPS - 1, False)]
    last = None
    for index, (step, theirs) in enumerate(parts):
        sums = [None, None]
        span(step, theirs, 0, FRONT, sums)
        if last is not None:
            keep(*last)
        span(step, theirs, FRONT, SEND, sums)
        if last is not None and last[1]:
            if last[0] == 0:
                @pl.when(core == 0)
                def _():
                    pl.semaphore_wait(go, 1)

            send(last[0])
        if index == STEPS - 2:
            span(step, theirs, SEND, MEET, sums)

            @pl.when(core == 1)
            def _():
                pl.semaphore_wait(barrier, SEATS - owner.astype(jnp.int32))
                pl.semaphore_signal(go, inc=1, device_id={"rows": partner}, device_id_type=MESH)

            for piece in range(3):
                swap(piece).wait()
            widen(other_wts, other_lines)
            span(step, theirs, MEET, pieces_all, sums)
        else:
            span(step, theirs, SEND, pieces_all, sums)
        last = step, theirs, False, sums
    span(STEPS - 1, True, 0, pieces_all, sums)
    keep(STEPS - 1, True, True, sums)
    send(STEPS - 1)

    def spread(target):
        return pltpu.make_async_remote_copy(
            src_ref=mine,
            dst_ref=out_ref.at[pl.ds(here, OCTET), :],
            send_sem=gather_send.at[0],
            recv_sem=gather_recv.at[0],
            device_id={"rows": target},
            device_id_type=MESH,
        )

    def spread_owners():
        first = mod(NX - x, NX) * NY + mod(NY - y, NY)
        for k in range(SEATS - 1):
            shift = mod(first + k, SEATS)
            shift = shift + (1 - div(shift + SEATS - 1, SEATS)) * mod(first + SEATS - 1, SEATS)
            yield spread(device(mod(x + div(shift, NY), NX), 0, mod(y + mod(shift, NY), NY), NC - 1))

    def spread_chip(px, py):
        for pz, pc in ((1, 1), (1, 0), (0, 0)):
            yield spread(device(px, pz, py, pc))

    def drain(ref, sem):
        return pltpu.make_async_copy(ref, ref, sem)

    here = pl.multiple_of((place_x * NY + place_y) * OCTET, OCTET)
    late = (0, 1, 2, 2)
    chips = sorted(((px, py) for px in range(NX) for py in range(NY)), key=lambda c: late[c[0]] + late[c[1]])

    @pl.when(keeps)
    def _():
        drain(inbox.at[pl.ds(0, 2 * (2 * STEPS - 1))], send_sem.at[0]).wait()

    @pl.when(jnp.logical_not(keeps))
    def _():
        drain(inbox.at[pl.ds(0, 4 * STEPS)], send_sem.at[0]).wait()

    @pl.when(owner)
    def _():
        drain(inbox.at[pl.ds(0, 2 * (SLOTS - OCTET))], recv_sem.at[0]).wait()
        sums = [None] * 4
        for s in range(2 * (SLOTS - OCTET)):
            sums[s % 4] = inbox[s] if sums[s % 4] is None else sums[s % 4] + inbox[s]

        @pl.when(keeps)
        def _():
            drain(inbox.at[pl.ds(0, 2 * (OCTET - 1))], recv_sem.at[1]).wait()

        @pl.when(jnp.logical_not(keeps))
        def _():
            drain(inbox.at[pl.ds(0, 2 * OCTET)], recv_sem.at[1]).wait()

        for s in range(2 * (SLOTS - OCTET), 2 * SLOTS):
            sums[s % 4] = sums[s % 4] + inbox[s]
        total = jnp.concatenate([sums[0] + sums[2], sums[1] + sums[3]], axis=0)

        p0 = total.astype(jnp.bfloat16).astype(jnp.float32)
        p1 = (total - p0).astype(jnp.bfloat16).astype(jnp.float32)
        p2 = total - p0 - p1
        split = jnp.concatenate([p0, p1, p2], axis=0).astype(jnp.bfloat16)
        sums3 = jnp.dot(split, prefix[...], preferred_element_type=jnp.float32)
        joined = sums3[:LEVELS] + sums3[LEVELS : 2 * LEVELS] + sums3[2 * LEVELS :]
        inner, level = joined[:, :LANES], joined[:, LANES:]
        inv = 1.0 / (total + 1.0)
        whole = jnp.sum(level, axis=0, keepdims=True)
        target = column_ref[...] * whole
        run = jnp.zeros((1, LANES), jnp.float32)
        acc = jnp.zeros((thr_ref.shape[1], LANES), jnp.float32)
        for h in range(LEVELS):
            before = inner[h : h + 1] + run
            run = run + level[h : h + 1]
            ratio = (target - before) * inv[h : h + 1]
            acc = acc + jnp.clip(ratio, 0.0, 1.0)
        turned = acc.T
        cuts = turned[:OCTET]
        for j in range(1, LANES // OCTET):
            cuts = cuts + turned[j * OCTET : (j + 1) * OCTET]
        mine[...] = cuts
        owners = list(spread_owners())
        others = [copy for px, py in chips for copy in spread_chip(px, py)]
        copies = owners[:1] + others[:18] + owners[1:] + others[18:]
        for copy in copies:
            copy.start()
        out_ref[pl.ds(here, OCTET), :] = cuts
        drain(inbox.at[pl.ds(0, RANKS - 1)], gather_send.at[0]).wait()
        drain(out_ref.at[pl.ds(0, (SEATS - 1) * OCTET), :], gather_recv.at[0]).wait()

    @pl.when(jnp.logical_not(owner))
    def _():
        drain(out_ref, gather_recv.at[0]).wait()


def solution(mesh):
    def local(bins, hessian, thresholds):
        words, width = bins.shape
        quantiles = thresholds.shape[0]
        return pl.pallas_call(
            kernel,
            out_shape=pltpu.VMEM((width, quantiles), jnp.float32),
            in_specs=[pl.BlockSpec(memory_space=pl.ANY)] * 3,
            out_specs=pl.BlockSpec(memory_space=pltpu.VMEM),
            scratch_shapes=[
                pltpu.VMEM((words, width), jnp.int32),
                pltpu.VMEM((4 * words // LANES, LANES), jnp.float32),
                pltpu.VMEM((1, quantiles), jnp.float32),
                pltpu.VMEM((LANES, 2 * LANES), jnp.bfloat16),
                pltpu.VMEM((quantiles, LANES), jnp.float32),
                pltpu.VMEM((width, words), jnp.int32),
                pltpu.VMEM((2, 4, GROUP, words), jnp.bfloat16),
                pltpu.VMEM((4, 2 * words // LANES, LANES), jnp.float32),
                pltpu.VMEM((width // 2, words), jnp.int32),
                pltpu.VMEM((2, 4, GROUP, words), jnp.bfloat16),
                pltpu.VMEM((4, 2 * words // LANES, LANES), jnp.float32),
                pltpu.VMEM((STEPS, 2, 2, OCTET, LANES), jnp.float32),
                pltpu.VMEM((STEPS, 2, 2, OCTET, LANES), jnp.float32),
                pltpu.VMEM((2 * SLOTS, OCTET, LANES), jnp.float32),
                pltpu.VMEM((OCTET, quantiles), jnp.float32),
                pltpu.SemaphoreType.DMA((words // LANES + 2,)),
                pltpu.SemaphoreType.DMA((3,)),
                pltpu.SemaphoreType.DMA((3,)),
                pltpu.SemaphoreType.DMA((1,)),
                pltpu.SemaphoreType.DMA((2,)),
                pltpu.SemaphoreType.DMA((1,)),
                pltpu.SemaphoreType.DMA((1,)),
                pltpu.SemaphoreType.REGULAR,
                pltpu.SemaphoreType.REGULAR,
            ],
            compiler_params=pltpu.CompilerParams(collective_id=0, has_side_effects=True),
        )(bins, hessian.reshape(-1, LANES), thresholds.reshape(1, -1))

    in_specs = (P("rows", "feat"), P("rows"), P())
    return jax.shard_map(local, mesh=mesh, in_specs=in_specs, out_specs=P("feat", None), check_vma=False)
```

```python
import jax
import jax.numpy as jnp
from jax import lax
from jax.experimental import pallas as pl
from jax.experimental.pallas import tpu as pltpu
from jax.sharding import PartitionSpec as P

LEVELS = 16
GROUP = 16
OCTET = 8
LANES = 128
CHUNK = 256
NX, NZ, NY, NC = 4, 2, 4, 2
RANKS = NX * NZ * NY * NC
SEATS = NX * NY
STEPS = 4
FRONT = 4
SEND = 8
MEET = 8
SLOTS = STEPS * OCTET
MESH = pl.DeviceIdType.MESH


def mod(value, size):
    return lax.rem(value, jnp.int32(size)) if isinstance(value, jax.Array) else value % size


def div(value, size):
    return lax.div(value, jnp.int32(size)) if isinstance(value, jax.Array) else value // size


def kernel(bins_hbm, hess_hbm, thr_hbm, out_ref, bins_ref, hess_ref, thr_ref, prefix, column_ref, cols, wts, lines, other_cols, other_wts, other_lines, partial, stage, inbox, mine, load_sem, swap_send, swap_recv, send_sem, recv_sem, gather_send, gather_recv, hello, go):
    words, width = bins_ref.shape
    tiles = words // LANES
    hess_load = pltpu.make_async_copy(hess_hbm, hess_ref, load_sem.at[tiles])
    hess_load.start()
    bins_loads = []
    for t in range(tiles):
        part = pl.ds(t * LANES, LANES)
        bins_loads.append(pltpu.make_async_copy(bins_hbm.at[part, :], bins_ref.at[part, :], load_sem.at[t]))
        bins_loads[t].start()
    thr_load = pltpu.make_async_copy(thr_hbm, thr_ref, load_sem.at[tiles + 1])
    thr_load.start()
    me = lax.axis_index("rows")
    x, z, y, core = div(me, NZ * NY * NC), mod(div(me, NY * NC), NZ), mod(div(me, NC), NY), mod(me, NC)
    owner = (core == NC - 1) & (z == 0)

    def device(px, pz, py, pc):
        return ((px * NZ + pz) * NY + py) * NC + pc

    partner = device(x, z, y, 1 - core)
    barrier = pltpu.get_barrier_semaphore()

    @pl.when(core == 1)
    def _():
        pl.semaphore_signal(barrier, inc=1, device_id={"rows": partner}, device_id_type=MESH)

    @pl.when(owner)
    def _():
        for step in range(NC, RANKS, NC):
            pl.semaphore_signal(barrier, inc=1, device_id={"rows": mod(me + step, RANKS)}, device_id_type=MESH)

    @pl.when(core == 0)
    def _():
        pl.semaphore_wait(barrier, 1)
        pl.semaphore_signal(hello, inc=1, device_id={"rows": partner}, device_id_type=MESH)

    src = lax.broadcasted_iota(jnp.int32, (LANES, LANES), 0)
    dst = lax.broadcasted_iota(jnp.int32, (LANES, LANES), 1)
    gap = dst - src
    same = jnp.bitwise_and(gap, OCTET - 1) == 0
    prefix[:, :LANES] = jnp.where(jnp.logical_and(same, gap > 0), 1.0, 0.0).astype(jnp.bfloat16)
    prefix[:, LANES:] = jnp.where(same, 1.0, 0.0).astype(jnp.bfloat16)

    quarter = LANES // 4
    order = jnp.where(src == 4 * (dst % quarter) + dst // quarter, 1.0, 0.0).astype(jnp.bfloat16)
    lane = lax.broadcasted_iota(jnp.int32, (2 * tiles, LANES), 1) // quarter
    hess_load.wait()
    flat = jnp.concatenate([hess_ref[pl.ds(j, tiles, stride=4), :] for j in range(4)], axis=0)
    left_factor = jnp.ones_like(flat)
    miss = jnp.abs(flat - flat.astype(jnp.bfloat16).astype(jnp.float32))
    for j in range(1, 128, 2):
        factor = 1.0 + j / 128.0
        other = (flat * (1.0 / factor)).astype(jnp.bfloat16).astype(jnp.float32)
        away = jnp.abs(flat - other * factor)
        left_factor = jnp.where(away < miss, factor, left_factor)
        miss = jnp.minimum(miss, away)
        if j == 63:
            for t in range(tiles // 2):
                bins_loads[t].wait()
            for t in range(tiles // 2):
                cols[:, t * LANES : (t + 1) * LANES] = bins_ref[t * LANES : (t + 1) * LANES, :].T
    right_factor = flat / left_factor
    for t in range(tiles // 2, tiles):
        bins_loads[t].wait()
    thr_load.wait()
    for t in range(tiles // 2, tiles):
        cols[:, t * LANES : (t + 1) * LANES] = bins_ref[t * LANES : (t + 1) * LANES, :].T
    half = width // 4

    def swap(piece):
        if piece < 2:
            there = pl.multiple_of(piece * 2 * half + (1 - core) * half, half)
            source, target = cols.at[pl.ds(there, half), :], other_cols.at[pl.ds(piece * half, half), :]
        else:
            source, target = lines, other_lines
        return pltpu.make_async_remote_copy(
            src_ref=source,
            dst_ref=target,
            send_sem=swap_send.at[piece],
            recv_sem=swap_recv.at[piece],
            device_id={"rows": partner},
            device_id_type=MESH,
        )

    @pl.when(core == 1)
    def _():
        pl.semaphore_wait(hello, 1)

    for piece in range(2):
        swap(piece).start()
    column_ref[...] = jnp.broadcast_to(thr_ref[...], (LANES, thr_ref.shape[1])).T
    pieces = jnp.concatenate([x[j * tiles : (j + 1) * tiles] for j in range(4) for x in (left_factor, right_factor)], axis=0)
    moved = jnp.dot(pieces.astype(jnp.bfloat16), order, preferred_element_type=jnp.float32)
    planes = []
    for k in range(4):
        plane = None
        for j in range(4):
            block = moved[2 * tiles * j : 2 * tiles * (j + 1)]
            if j != k:
                block = pltpu.roll(block, (quarter * (j - k)) % LANES, 1)
            plane = block if plane is None else jnp.where(lane == j, block, plane)
        lines[k] = plane
        planes.append(plane)

    def widen(target, source):
        for k in range(4):
            plane = source[k]
            for piece in range(2):
                for t in range(tiles):
                    line = plane[piece * tiles + t : piece * tiles + t + 1]
                    target[piece, k, :, t * LANES : (t + 1) * LANES] = jnp.broadcast_to(line, (GROUP, LANES)).astype(jnp.bfloat16)

    swap(2).start()
    widen(wts, planes)

    sub = lax.broadcasted_iota(jnp.int32, (OCTET, LANES), 0)
    diagonal = sub == lax.broadcasted_iota(jnp.int32, (OCTET, LANES), 1) % OCTET

    def gather_rows(tiles8):
        low4, low2, low1 = sub < 4, sub % 4 < 2, sub % 2 < 1
        four = []
        for a in range(4):
            p, q = tiles8[a], tiles8[a + 4]
            four.append(jnp.where(low4, p, q) + pltpu.roll(jnp.where(low4, q, p), 4, 0))
        two = []
        for a in range(2):
            p, q = four[a], four[a + 2]
            two.append(jnp.where(low2, p, q) + jnp.where(low2, pltpu.roll(p, 6, 0), pltpu.roll(q, 2, 0)))
        p, q = two
        return jnp.where(low1, p, q) + jnp.where(low1, pltpu.roll(p, 7, 0), pltpu.roll(q, 1, 0))

    def products(columns, weights, base, first, last, sums):
        zero = jnp.zeros((GROUP, CHUNK), jnp.bfloat16)
        upper = lax.broadcasted_iota(jnp.int32, (GROUP, CHUNK), 0) // OCTET
        for index in range(first, last):
            c, k = index // 4, index % 4
            part = columns[pl.ds(base, GROUP), c * CHUNK : (c + 1) * CHUNK]
            high = jnp.bitwise_and(jnp.right_shift(part, 8 * k + 4), 15).astype(jnp.float32).astype(jnp.bfloat16)
            low = jnp.bitwise_and(jnp.right_shift(part, 8 * k), 15)
            w0 = weights[0, k, :, c * CHUNK : (c + 1) * CHUNK]
            w1 = weights[1, k, :, c * CHUNK : (c + 1) * CHUNK]
            left = jnp.concatenate([jnp.where(high == jnp.bfloat16(h), w0, zero) for h in range(LEVELS)], axis=0)
            rights = []
            for o in range(2):
                eight = low[o * OCTET : (o + 1) * OCTET]
                pair = (jnp.concatenate([eight, eight], axis=0) - upper).astype(jnp.float32).astype(jnp.bfloat16)
                rights += [jnp.where(pair == jnp.bfloat16(l), w1, zero) for l in range(0, LEVELS, 2)]
            right = jnp.concatenate(rights, axis=0)
            part_sum = lax.dot_general(left, right, (((1,), (1,)), ((), ())), preferred_element_type=jnp.float32)
            side = index % 2
            sums[side] = part_sum if sums[side] is None else sums[side] + part_sum

    def extract(sums):
        blocks = []
        for o in range(2):
            cut = slice(o * LANES, (o + 1) * LANES)
            rows = []
            for h in range(LEVELS):
                pick = slice(h * GROUP + o * OCTET, h * GROUP + (o + 1) * OCTET)
                rows.append(jnp.where(diagonal, sums[0][pick, cut], 0.0) + jnp.where(diagonal, sums[1][pick, cut], 0.0))
            blocks.append([gather_rows(rows[:8]), gather_rows(rows[8:])])
        return blocks

    place_x, place_y = mod(x + 1, NX), mod(y + 1, NY)

    def block_of(step):
        return mod(div(place_x, 2) + (1 if step < 2 else 0), 2), mod(div(place_y, 2) + (1 if step % 2 == 0 else 0), 2)

    def outgoing(step, o):
        block_x, block_y = block_of(step)
        target = device(mod(2 * block_x + core + NX - 1, NX), 0, mod(2 * block_y + o + NY - 1, NY), NC - 1)
        return pltpu.make_async_remote_copy(
            src_ref=stage.at[step, o],
            dst_ref=inbox.at[pl.ds(2 * (step * OCTET + mod(place_x, 2) * 4 + mod(place_y, 2) * 2 + z), 2)],
            send_sem=send_sem.at[0],
            recv_sem=recv_sem.at[step // (STEPS - 1)],
            device_id={"rows": target},
            device_id_type=MESH,
        )

    pieces_all = words // CHUNK * 4
    keeps = owner & (mod(place_x, 2) == core)

    def keep(step, theirs, alone, sums):
        for o, block in enumerate(extract(sums)):
            for part in range(2):
                if not theirs:
                    partial[step, o, part] = block[part]
                else:
                    stage[step, o, part] = block[part] if alone else block[part] + partial[step, o, part]

    def send(step):
        for o in range(2):
            if step < STEPS - 1:
                outgoing(step, o).start()
            else:
                own = keeps & (mod(place_y, 2) == o)

                @pl.when(own)
                def _():
                    inbox[pl.ds(2 * (step * OCTET + mod(place_x, 2) * 4 + o * 2), 2)] = stage[step, o]

                @pl.when(jnp.logical_not(own))
                def _():
                    outgoing(step, o).start()

    def span(step, theirs, first, last, sums):
        block_x, block_y = block_of(step)
        if theirs:
            base = pl.multiple_of(block_x * half + block_y * GROUP, GROUP)
            products(other_cols, other_wts, base, first, last, sums)
        else:
            base = pl.multiple_of((2 * block_x + core) * half + block_y * GROUP, GROUP)
            products(cols, wts, base, first, last, sums)

    parts = [(step, theirs) for theirs in (False, True) for step in range(STEPS - 1)] + [(STEPS - 1, False)]
    last = None
    for index, (step, theirs) in enumerate(parts):
        sums = [None, None]
        span(step, theirs, 0, FRONT, sums)
        if last is not None:
            keep(*last)
        span(step, theirs, FRONT, SEND, sums)
        if last is not None and last[1]:
            if last[0] == 0:
                @pl.when(core == 0)
                def _():
                    pl.semaphore_wait(go, 1)

            send(last[0])
        if index == STEPS - 2:
            span(step, theirs, SEND, MEET, sums)

            @pl.when(core == 1)
            def _():
                pl.semaphore_wait(barrier, SEATS - owner.astype(jnp.int32))
                pl.semaphore_signal(go, inc=1, device_id={"rows": partner}, device_id_type=MESH)

            for piece in range(3):
                swap(piece).wait()
            widen(other_wts, other_lines)
            span(step, theirs, MEET, pieces_all, sums)
        else:
            span(step, theirs, SEND, pieces_all, sums)
        last = step, theirs, False, sums
    span(STEPS - 1, True, 0, pieces_all, sums)
    keep(STEPS - 1, True, True, sums)
    send(STEPS - 1)

    def spread(target):
        return pltpu.make_async_remote_copy(
            src_ref=mine,
            dst_ref=out_ref.at[pl.ds(here, OCTET), :],
            send_sem=gather_send.at[0],
            recv_sem=gather_recv.at[0],
            device_id={"rows": target},
            device_id_type=MESH,
        )

    def spread_owners():
        first = mod(NX - x, NX) * NY + mod(NY - y, NY)
        for k in range(SEATS - 1):
            shift = mod(first + k, SEATS)
            shift = shift + (1 - div(shift + SEATS - 1, SEATS)) * mod(first + SEATS - 1, SEATS)
            yield spread(device(mod(x + div(shift, NY), NX), 0, mod(y + mod(shift, NY), NY), NC - 1))

    def spread_chip(px, py):
        for pz, pc in ((1, 1), (1, 0), (0, 0)):
            yield spread(device(px, pz, py, pc))

    def drain(ref, sem):
        return pltpu.make_async_copy(ref, ref, sem)

    here = pl.multiple_of((place_x * NY + place_y) * OCTET, OCTET)
    late = (0, 1, 2, 2)
    chips = sorted(((px, py) for px in range(NX) for py in range(NY)), key=lambda c: late[c[0]] + late[c[1]])

    @pl.when(keeps)
    def _():
        drain(inbox.at[pl.ds(0, 2 * (2 * STEPS - 1))], send_sem.at[0]).wait()

    @pl.when(jnp.logical_not(keeps))
    def _():
        drain(inbox.at[pl.ds(0, 4 * STEPS)], send_sem.at[0]).wait()

    @pl.when(owner)
    def _():
        drain(inbox.at[pl.ds(0, 2 * (SLOTS - OCTET))], recv_sem.at[0]).wait()
        sums = [None] * 4
        for s in range(2 * (SLOTS - OCTET)):
            sums[s % 4] = inbox[s] if sums[s % 4] is None else sums[s % 4] + inbox[s]

        @pl.when(keeps)
        def _():
            drain(inbox.at[pl.ds(0, 2 * (OCTET - 1))], recv_sem.at[1]).wait()

        @pl.when(jnp.logical_not(keeps))
        def _():
            drain(inbox.at[pl.ds(0, 2 * OCTET)], recv_sem.at[1]).wait()

        for s in range(2 * (SLOTS - OCTET), 2 * SLOTS):
            sums[s % 4] = sums[s % 4] + inbox[s]
        total = jnp.concatenate([sums[0] + sums[2], sums[1] + sums[3]], axis=0)

        p0 = total.astype(jnp.bfloat16).astype(jnp.float32)
        p1 = (total - p0).astype(jnp.bfloat16).astype(jnp.float32)
        p2 = total - p0 - p1
        split = jnp.concatenate([p0, p1, p2], axis=0).astype(jnp.bfloat16)
        sums3 = jnp.dot(split, prefix[...], preferred_element_type=jnp.float32)
        joined = sums3[:LEVELS] + sums3[LEVELS : 2 * LEVELS] + sums3[2 * LEVELS :]
        inner, level = joined[:, :LANES], joined[:, LANES:]
        inv = 1.0 / (total + 1.0)
        whole = jnp.sum(level, axis=0, keepdims=True)
        target = column_ref[...] * whole
        run = jnp.zeros((1, LANES), jnp.float32)
        acc = jnp.zeros((thr_ref.shape[1], LANES), jnp.float32)
        for h in range(LEVELS):
            before = inner[h : h + 1] + run
            run = run + level[h : h + 1]
            ratio = (target - before) * inv[h : h + 1]
            acc = acc + jnp.clip(ratio, 0.0, 1.0)
        turned = acc.T
        cuts = turned[:OCTET]
        for j in range(1, LANES // OCTET):
            cuts = cuts + turned[j * OCTET : (j + 1) * OCTET]
        mine[...] = cuts
        owners = list(spread_owners())
        others = [copy for px, py in chips for copy in spread_chip(px, py)]
        copies = owners[:1] + others[:18] + owners[1:] + others[18:]
        for copy in copies:
            copy.start()
        out_ref[pl.ds(here, OCTET), :] = cuts
        drain(inbox.at[pl.ds(0, RANKS - 1)], gather_send.at[0]).wait()
        drain(out_ref.at[pl.ds(0, (SEATS - 1) * OCTET), :], gather_recv.at[0]).wait()

    @pl.when(jnp.logical_not(owner))
    def _():
        drain(out_ref, gather_recv.at[0]).wait()


def solution(mesh):
    def local(bins, hessian, thresholds):
        words, width = bins.shape
        quantiles = thresholds.shape[0]
        return pl.pallas_call(
            kernel,
            out_shape=pltpu.VMEM((width, quantiles), jnp.float32),
            in_specs=[pl.BlockSpec(memory_space=pl.ANY)] * 3,
            out_specs=pl.BlockSpec(memory_space=pltpu.VMEM),
            scratch_shapes=[
                pltpu.VMEM((words, width), jnp.int32),
                pltpu.VMEM((4 * words // LANES, LANES), jnp.float32),
                pltpu.VMEM((1, quantiles), jnp.float32),
                pltpu.VMEM((LANES, 2 * LANES), jnp.bfloat16),
                pltpu.VMEM((quantiles, LANES), jnp.float32),
                pltpu.VMEM((width, words), jnp.int32),
                pltpu.VMEM((2, 4, GROUP, words), jnp.bfloat16),
                pltpu.VMEM((4, 2 * words // LANES, LANES), jnp.float32),
                pltpu.VMEM((width // 2, words), jnp.int32),
                pltpu.VMEM((2, 4, GROUP, words), jnp.bfloat16),
                pltpu.VMEM((4, 2 * words // LANES, LANES), jnp.float32),
                pltpu.VMEM((STEPS, 2, 2, OCTET, LANES), jnp.float32),
                pltpu.VMEM((STEPS, 2, 2, OCTET, LANES), jnp.float32),
                pltpu.VMEM((2 * SLOTS, OCTET, LANES), jnp.float32),
                pltpu.VMEM((OCTET, quantiles), jnp.float32),
                pltpu.SemaphoreType.DMA((words // LANES + 2,)),
                pltpu.SemaphoreType.DMA((3,)),
                pltpu.SemaphoreType.DMA((3,)),
                pltpu.SemaphoreType.DMA((1,)),
                pltpu.SemaphoreType.DMA((2,)),
                pltpu.SemaphoreType.DMA((1,)),
                pltpu.SemaphoreType.DMA((1,)),
                pltpu.SemaphoreType.REGULAR,
                pltpu.SemaphoreType.REGULAR,
            ],
            compiler_params=pltpu.CompilerParams(collective_id=0, has_side_effects=True),
        )(bins, hessian.reshape(-1, LANES), thresholds.reshape(1, -1))

    in_specs = (P("rows", "feat"), P("rows"), P())
    return jax.shard_map(local, mesh=mesh, in_specs=in_specs, out_specs=P("feat", None), check_vma=False)
```

```python
import jax
import jax.numpy as jnp
from jax import lax
from jax.experimental import pallas as pl
from jax.experimental.pallas import tpu as pltpu
from jax.sharding import PartitionSpec as P

LEVELS = 16
GROUP = 16
OCTET = 8
LANES = 128
CHUNK = 256
NX, NZ, NY, NC = 4, 2, 4, 2
RANKS = NX * NZ * NY * NC
SEATS = NX * NY
STEPS = 4
FRONT = 4
SEND = 8
MEET = 8
SLOTS = STEPS * OCTET
MESH = pl.DeviceIdType.MESH


def mod(value, size):
    return lax.rem(value, jnp.int32(size)) if isinstance(value, jax.Array) else value % size


def div(value, size):
    return lax.div(value, jnp.int32(size)) if isinstance(value, jax.Array) else value // size


def kernel(bins_hbm, hess_hbm, thr_hbm, out_ref, bins_ref, hess_ref, thr_ref, prefix, column_ref, cols, wts, lines, other_cols, other_wts, other_lines, partial, stage, inbox, mine, load_sem, swap_send, swap_recv, send_sem, recv_sem, gather_send, gather_recv, hello, go):
    words, width = bins_ref.shape
    tiles = words // LANES
    hess_load = pltpu.make_async_copy(hess_hbm, hess_ref, load_sem.at[tiles])
    hess_load.start()
    bins_loads = []
    for t in range(tiles):
        part = pl.ds(t * LANES, LANES)
        bins_loads.append(pltpu.make_async_copy(bins_hbm.at[part, :], bins_ref.at[part, :], load_sem.at[t]))
        bins_loads[t].start()
    thr_load = pltpu.make_async_copy(thr_hbm, thr_ref, load_sem.at[tiles + 1])
    thr_load.start()
    me = lax.axis_index("rows")
    x, z, y, core = div(me, NZ * NY * NC), mod(div(me, NY * NC), NZ), mod(div(me, NC), NY), mod(me, NC)
    owner = (core == NC - 1) & (z == 0)

    def device(px, pz, py, pc):
        return ((px * NZ + pz) * NY + py) * NC + pc

    partner = device(x, z, y, 1 - core)
    barrier = pltpu.get_barrier_semaphore()

    @pl.when(core == 1)
    def _():
        pl.semaphore_signal(barrier, inc=1, device_id={"rows": partner}, device_id_type=MESH)

    @pl.when(owner)
    def _():
        for step in range(NC, RANKS, NC):
            pl.semaphore_signal(barrier, inc=1, device_id={"rows": mod(me + step, RANKS)}, device_id_type=MESH)

    @pl.when(core == 0)
    def _():
        pl.semaphore_wait(barrier, 1)
        pl.semaphore_signal(hello, inc=1, device_id={"rows": partner}, device_id_type=MESH)

    src = lax.broadcasted_iota(jnp.int32, (LANES, LANES), 0)
    dst = lax.broadcasted_iota(jnp.int32, (LANES, LANES), 1)
    gap = dst - src
    same = jnp.bitwise_and(gap, OCTET - 1) == 0
    prefix[:, :LANES] = jnp.where(jnp.logical_and(same, gap > 0), 1.0, 0.0).astype(jnp.bfloat16)
    prefix[:, LANES:] = jnp.where(same, 1.0, 0.0).astype(jnp.bfloat16)

    quarter = LANES // 4
    order = jnp.where(src == 4 * (dst % quarter) + dst // quarter, 1.0, 0.0).astype(jnp.bfloat16)
    lane = lax.broadcasted_iota(jnp.int32, (2 * tiles, LANES), 1) // quarter
    hess_load.wait()
    flat = jnp.concatenate([hess_ref[pl.ds(j, tiles, stride=4), :] for j in range(4)], axis=0)
    left_factor = jnp.ones_like(flat)
    miss = jnp.abs(flat - flat.astype(jnp.bfloat16).astype(jnp.float32))
    for j in range(1, 128, 2):
        factor = 1.0 + j / 128.0
        other = (flat * (1.0 / factor)).astype(jnp.bfloat16).astype(jnp.float32)
        away = jnp.abs(flat - other * factor)
        left_factor = jnp.where(away < miss, factor, left_factor)
        miss = jnp.minimum(miss, away)
        if j == 63:
            for t in range(tiles // 2):
                bins_loads[t].wait()
            for t in range(tiles // 2):
                cols[:, t * LANES : (t + 1) * LANES] = bins_ref[t * LANES : (t + 1) * LANES, :].T
    right_factor = flat / left_factor
    for t in range(tiles // 2, tiles):
        bins_loads[t].wait()
    thr_load.wait()
    for t in range(tiles // 2, tiles):
        cols[:, t * LANES : (t + 1) * LANES] = bins_ref[t * LANES : (t + 1) * LANES, :].T
    column_ref[...] = jnp.broadcast_to(thr_ref[...], (LANES, thr_ref.shape[1])).T
    pieces = jnp.concatenate([x[j * tiles : (j + 1) * tiles] for j in range(4) for x in (left_factor, right_factor)], axis=0)
    moved = jnp.dot(pieces.astype(jnp.bfloat16), order, preferred_element_type=jnp.float32)
    planes = []
    for k in range(4):
        plane = None
        for j in range(4):
            block = moved[2 * tiles * j : 2 * tiles * (j + 1)]
            if j != k:
                block = pltpu.roll(block, (quarter * (j - k)) % LANES, 1)
            plane = block if plane is None else jnp.where(lane == j, block, plane)
        lines[k] = plane
        planes.append(plane)

    def widen(target, source):
        for k in range(4):
            plane = source[k]
            for piece in range(2):
                for t in range(tiles):
                    line = plane[piece * tiles + t : piece * tiles + t + 1]
                    target[piece, k, :, t * LANES : (t + 1) * LANES] = jnp.broadcast_to(line, (GROUP, LANES)).astype(jnp.bfloat16)

    half = width // 4

    def swap(piece):
        if piece < 2:
            there = pl.multiple_of(piece * 2 * half + (1 - core) * half, half)
            source, target = cols.at[pl.ds(there, half), :], other_cols.at[pl.ds(piece * half, half), :]
        else:
            source, target = lines, other_lines
        return pltpu.make_async_remote_copy(
            src_ref=source,
            dst_ref=target,
            send_sem=swap_send.at[piece],
            recv_sem=swap_recv.at[piece],
            device_id={"rows": partner},
            device_id_type=MESH,
        )

    @pl.when(core == 1)
    def _():
        pl.semaphore_wait(hello, 1)

    for piece in (2, 0, 1):
        swap(piece).start()
    widen(wts, planes)

    sub = lax.broadcasted_iota(jnp.int32, (OCTET, LANES), 0)
    diagonal = sub == lax.broadcasted_iota(jnp.int32, (OCTET, LANES), 1) % OCTET

    def gather_rows(tiles8):
        low4, low2, low1 = sub < 4, sub % 4 < 2, sub % 2 < 1
        four = []
        for a in range(4):
            p, q = tiles8[a], tiles8[a + 4]
            four.append(jnp.where(low4, p, q) + pltpu.roll(jnp.where(low4, q, p), 4, 0))
        two = []
        for a in range(2):
            p, q = four[a], four[a + 2]
            two.append(jnp.where(low2, p, q) + jnp.where(low2, pltpu.roll(p, 6, 0), pltpu.roll(q, 2, 0)))
        p, q = two
        return jnp.where(low1, p, q) + jnp.where(low1, pltpu.roll(p, 7, 0), pltpu.roll(q, 1, 0))

    def products(columns, weights, base, first, last, sums):
        zero = jnp.zeros((GROUP, CHUNK), jnp.bfloat16)
        upper = lax.broadcasted_iota(jnp.int32, (GROUP, CHUNK), 0) // OCTET
        for index in range(first, last):
            c, k = index // 4, index % 4
            part = columns[pl.ds(base, GROUP), c * CHUNK : (c + 1) * CHUNK]
            high = jnp.bitwise_and(jnp.right_shift(part, 8 * k + 4), 15).astype(jnp.float32).astype(jnp.bfloat16)
            low = jnp.bitwise_and(jnp.right_shift(part, 8 * k), 15)
            w0 = weights[0, k, :, c * CHUNK : (c + 1) * CHUNK]
            w1 = weights[1, k, :, c * CHUNK : (c + 1) * CHUNK]
            left = jnp.concatenate([jnp.where(high == jnp.bfloat16(h), w0, zero) for h in range(LEVELS)], axis=0)
            rights = []
            for o in range(2):
                eight = low[o * OCTET : (o + 1) * OCTET]
                pair = (jnp.concatenate([eight, eight], axis=0) - upper).astype(jnp.float32).astype(jnp.bfloat16)
                rights += [jnp.where(pair == jnp.bfloat16(l), w1, zero) for l in range(0, LEVELS, 2)]
            right = jnp.concatenate(rights, axis=0)
            part_sum = lax.dot_general(left, right, (((1,), (1,)), ((), ())), preferred_element_type=jnp.float32)
            side = index % 2
            sums[side] = part_sum if sums[side] is None else sums[side] + part_sum

    def extract(sums):
        blocks = []
        for o in range(2):
            cut = slice(o * LANES, (o + 1) * LANES)
            rows = []
            for h in range(LEVELS):
                pick = slice(h * GROUP + o * OCTET, h * GROUP + (o + 1) * OCTET)
                rows.append(jnp.where(diagonal, sums[0][pick, cut], 0.0) + jnp.where(diagonal, sums[1][pick, cut], 0.0))
            blocks.append([gather_rows(rows[:8]), gather_rows(rows[8:])])
        return blocks

    place_x, place_y = mod(x + 1, NX), mod(y + 1, NY)

    def block_of(step):
        return mod(div(place_x, 2) + (1 if step < 2 else 0), 2), mod(div(place_y, 2) + (1 if step % 2 == 0 else 0), 2)

    def outgoing(step, o):
        block_x, block_y = block_of(step)
        target = device(mod(2 * block_x + core + NX - 1, NX), 0, mod(2 * block_y + o + NY - 1, NY), NC - 1)
        return pltpu.make_async_remote_copy(
            src_ref=stage.at[step, o],
            dst_ref=inbox.at[pl.ds(2 * (step * OCTET + mod(place_x, 2) * 4 + mod(place_y, 2) * 2 + z), 2)],
            send_sem=send_sem.at[0],
            recv_sem=recv_sem.at[step // (STEPS - 1)],
            device_id={"rows": target},
            device_id_type=MESH,
        )

    pieces_all = words // CHUNK * 4
    keeps = owner & (mod(place_x, 2) == core)

    def keep(step, theirs, alone, sums):
        for o, block in enumerate(extract(sums)):
            for part in range(2):
                if not theirs:
                    partial[step, o, part] = block[part]
                else:
                    stage[step, o, part] = block[part] if alone else block[part] + partial[step, o, part]

    def send(step):
        for o in range(2):
            if step < STEPS - 1:
                outgoing(step, o).start()
            else:
                own = keeps & (mod(place_y, 2) == o)

                @pl.when(own)
                def _():
                    inbox[pl.ds(2 * (step * OCTET + mod(place_x, 2) * 4 + o * 2), 2)] = stage[step, o]

                @pl.when(jnp.logical_not(own))
                def _():
                    outgoing(step, o).start()

    def span(step, theirs, first, last, sums):
        block_x, block_y = block_of(step)
        if theirs:
            base = pl.multiple_of(block_x * half + block_y * GROUP, GROUP)
            products(other_cols, other_wts, base, first, last, sums)
        else:
            base = pl.multiple_of((2 * block_x + core) * half + block_y * GROUP, GROUP)
            products(cols, wts, base, first, last, sums)

    parts = [(step, theirs) for theirs in (False, True) for step in range(STEPS - 1)] + [(STEPS - 1, False)]
    last = None
    for index, (step, theirs) in enumerate(parts):
        sums = [None, None]
        span(step, theirs, 0, FRONT, sums)
        if last is not None:
            keep(*last)
        span(step, theirs, FRONT, SEND, sums)
        if last is not None and last[1]:
            if last[0] == 0:
                @pl.when(core == 0)
                def _():
                    pl.semaphore_wait(go, 1)

            send(last[0])
        if index == STEPS - 2:
            span(step, theirs, SEND, MEET, sums)

            @pl.when(core == 1)
            def _():
                pl.semaphore_wait(barrier, SEATS - owner.astype(jnp.int32))
                pl.semaphore_signal(go, inc=1, device_id={"rows": partner}, device_id_type=MESH)

            for piece in range(3):
                swap(piece).wait()
            widen(other_wts, other_lines)
            span(step, theirs, MEET, pieces_all, sums)
        else:
            span(step, theirs, SEND, pieces_all, sums)
        last = step, theirs, False, sums
    span(STEPS - 1, True, 0, pieces_all, sums)
    keep(STEPS - 1, True, True, sums)
    send(STEPS - 1)

    def spread(target):
        return pltpu.make_async_remote_copy(
            src_ref=mine,
            dst_ref=out_ref.at[pl.ds(here, OCTET), :],
            send_sem=gather_send.at[0],
            recv_sem=gather_recv.at[0],
            device_id={"rows": target},
            device_id_type=MESH,
        )

    def spread_owners():
        first = mod(NX - x, NX) * NY + mod(NY - y, NY)
        for k in range(SEATS - 1):
            shift = mod(first + k, SEATS)
            shift = shift + (1 - div(shift + SEATS - 1, SEATS)) * mod(first + SEATS - 1, SEATS)
            yield spread(device(mod(x + div(shift, NY), NX), 0, mod(y + mod(shift, NY), NY), NC - 1))

    def spread_chip(px, py):
        for pz, pc in ((1, 1), (1, 0), (0, 0)):
            yield spread(device(px, pz, py, pc))

    def drain(ref, sem):
        return pltpu.make_async_copy(ref, ref, sem)

    here = pl.multiple_of((place_x * NY + place_y) * OCTET, OCTET)
    late = (0, 1, 2, 2)
    chips = sorted(((px, py) for px in range(NX) for py in range(NY)), key=lambda c: late[c[0]] + late[c[1]])

    @pl.when(keeps)
    def _():
        drain(inbox.at[pl.ds(0, 2 * (2 * STEPS - 1))], send_sem.at[0]).wait()

    @pl.when(jnp.logical_not(keeps))
    def _():
        drain(inbox.at[pl.ds(0, 4 * STEPS)], send_sem.at[0]).wait()

    @pl.when(owner)
    def _():
        drain(inbox.at[pl.ds(0, 2 * (SLOTS - OCTET))], recv_sem.at[0]).wait()
        sums = [None] * 4
        for s in range(2 * (SLOTS - OCTET)):
            sums[s % 4] = inbox[s] if sums[s % 4] is None else sums[s % 4] + inbox[s]

        @pl.when(keeps)
        def _():
            drain(inbox.at[pl.ds(0, 2 * (OCTET - 1))], recv_sem.at[1]).wait()

        @pl.when(jnp.logical_not(keeps))
        def _():
            drain(inbox.at[pl.ds(0, 2 * OCTET)], recv_sem.at[1]).wait()

        for s in range(2 * (SLOTS - OCTET), 2 * SLOTS):
            sums[s % 4] = sums[s % 4] + inbox[s]
        total = jnp.concatenate([sums[0] + sums[2], sums[1] + sums[3]], axis=0)

        p0 = total.astype(jnp.bfloat16).astype(jnp.float32)
        p1 = (total - p0).astype(jnp.bfloat16).astype(jnp.float32)
        p2 = total - p0 - p1
        split = jnp.concatenate([p0, p1, p2], axis=0).astype(jnp.bfloat16)
        sums3 = jnp.dot(split, prefix[...], preferred_element_type=jnp.float32)
        joined = sums3[:LEVELS] + sums3[LEVELS : 2 * LEVELS] + sums3[2 * LEVELS :]
        inner, level = joined[:, :LANES], joined[:, LANES:]
        inv = 1.0 / (total + 1.0)
        whole = jnp.sum(level, axis=0, keepdims=True)
        target = column_ref[...] * whole
        run = jnp.zeros((1, LANES), jnp.float32)
        acc = jnp.zeros((thr_ref.shape[1], LANES), jnp.float32)
        for h in range(LEVELS):
            before = inner[h : h + 1] + run
            run = run + level[h : h + 1]
            ratio = (target - before) * inv[h : h + 1]
            acc = acc + jnp.clip(ratio, 0.0, 1.0)
        turned = acc.T
        cuts = turned[:OCTET]
        for j in range(1, LANES // OCTET):
            cuts = cuts + turned[j * OCTET : (j + 1) * OCTET]
        mine[...] = cuts
        owners = list(spread_owners())
        others = [copy for px, py in chips for copy in spread_chip(px, py)]
        copies = owners[:1] + others[:18] + owners[1:] + others[18:]
        for copy in copies:
            copy.start()
        out_ref[pl.ds(here, OCTET), :] = cuts
        drain(inbox.at[pl.ds(0, RANKS - 1)], gather_send.at[0]).wait()
        drain(out_ref.at[pl.ds(0, (SEATS - 1) * OCTET), :], gather_recv.at[0]).wait()

    @pl.when(jnp.logical_not(owner))
    def _():
        drain(out_ref, gather_recv.at[0]).wait()


def solution(mesh):
    def local(bins, hessian, thresholds):
        words, width = bins.shape
        quantiles = thresholds.shape[0]
        return pl.pallas_call(
            kernel,
            out_shape=pltpu.VMEM((width, quantiles), jnp.float32),
            in_specs=[pl.BlockSpec(memory_space=pl.ANY)] * 3,
            out_specs=pl.BlockSpec(memory_space=pltpu.VMEM),
            scratch_shapes=[
                pltpu.VMEM((words, width), jnp.int32),
                pltpu.VMEM((4 * words // LANES, LANES), jnp.float32),
                pltpu.VMEM((1, quantiles), jnp.float32),
                pltpu.VMEM((LANES, 2 * LANES), jnp.bfloat16),
                pltpu.VMEM((quantiles, LANES), jnp.float32),
                pltpu.VMEM((width, words), jnp.int32),
                pltpu.VMEM((2, 4, GROUP, words), jnp.bfloat16),
                pltpu.VMEM((4, 2 * words // LANES, LANES), jnp.float32),
                pltpu.VMEM((width // 2, words), jnp.int32),
                pltpu.VMEM((2, 4, GROUP, words), jnp.bfloat16),
                pltpu.VMEM((4, 2 * words // LANES, LANES), jnp.float32),
                pltpu.VMEM((STEPS, 2, 2, OCTET, LANES), jnp.float32),
                pltpu.VMEM((STEPS, 2, 2, OCTET, LANES), jnp.float32),
                pltpu.VMEM((2 * SLOTS, OCTET, LANES), jnp.float32),
                pltpu.VMEM((OCTET, quantiles), jnp.float32),
                pltpu.SemaphoreType.DMA((words // LANES + 2,)),
                pltpu.SemaphoreType.DMA((3,)),
                pltpu.SemaphoreType.DMA((3,)),
                pltpu.SemaphoreType.DMA((1,)),
                pltpu.SemaphoreType.DMA((2,)),
                pltpu.SemaphoreType.DMA((1,)),
                pltpu.SemaphoreType.DMA((1,)),
                pltpu.SemaphoreType.REGULAR,
                pltpu.SemaphoreType.REGULAR,
            ],
            compiler_params=pltpu.CompilerParams(collective_id=0, has_side_effects=True),
        )(bins, hessian.reshape(-1, LANES), thresholds.reshape(1, -1))

    in_specs = (P("rows", "feat"), P("rows"), P())
    return jax.shard_map(local, mesh=mesh, in_specs=in_specs, out_specs=P("feat", None), check_vma=False)
```
